128 devices in a mesh: leaf: 16 (over x, z), rows: 8 (over y, core).
Axes of the slice: x: 4, y: 4, z: 4, core: 2. Of those that a mesh axis runs over, the one named last changes fastest.
Arguments:
- loads_first: bfloat16 [98304, 256], P(('leaf', 'rows')), may hold values from -6 to 6
- loads_second: bfloat16 [49152, 256], P(('leaf', 'rows')), may hold values from -6 to 6
- loads_third: bfloat16 [24576, 256], P(('leaf', 'rows')), may hold values from -6 to 6
- loads_fourth: bfloat16 [12288, 256], P(('leaf', 'rows')), may hold values from -6 to 6
- inverse_first: bfloat16 [98304, 6144], P(('leaf', 'rows')), as said below
- inverse_second: bfloat16 [49152, 6144], P(('leaf', 'rows')), as said below
- inverse_third: bfloat16 [24576, 6144], P(('leaf', 'rows')), as said below
- inverse_fourth: bfloat16 [12288, 6144], P(('leaf', 'rows')), as said below
- panel_first: bfloat16 [1536, 98304], P(None, ('leaf', 'rows')), may hold values from -0.078125 to 0.078125
- panel_second: bfloat16 [1536, 49152], P(None, ('leaf', 'rows')), may hold values from -0.078125 to 0.078125
- panel_third: bfloat16 [1536, 24576], P(None, ('leaf', 'rows')), may hold values from -0.078125 to 0.078125
- panel_fourth: bfloat16 [1536, 12288], P(None, ('leaf', 'rows')), may hold values from -0.078125 to 0.078125
- blocks_first: int32 [16, 12], replicated, may hold values from 0 to 47, as said below
- blocks_second: int32 [8, 12], replicated, may hold values from 0 to 47, as said below
- blocks_third: int32 [4, 12], replicated, may hold values from 0 to 47, as said below
Outputs:
- solved_first: bfloat16 [98304, 256], P(('leaf', 'rows'))
- solved_second: bfloat16 [49152, 256], P(('leaf', 'rows'))
- solved_third: bfloat16 [24576, 256], P(('leaf', 'rows'))
- solved_fourth: bfloat16 [12288, 256], P(('leaf', 'rows'))
- ancestor_update: float32 [3072, 256], P(('leaf', 'rows'))
The draws below stay inside these ranges and needn't reach their ends.
Inputs may be any that keep to these rules, and one draw needn't show every extreme that they name: `blocks_first`: each row lists 12 distinct block numbers in increasing order. `blocks_second`: each row lists 12 distinct block numbers in increasing order. `blocks_third`: each row lists 12 distinct block numbers in increasing order. `inverse_first`: each block of 6144 rows is lower triangular with a positive diagonal. `inverse_second`: each block of 6144 rows is lower triangular with a positive diagonal. `inverse_third`: each block of 6144 rows is lower triangular with a positive diagonal. `inverse_fourth`: each block of 6144 rows is lower triangular with a positive diagonal.
All inputs are finite; a program needn't handle non-finite values.
Results may differ from the reference program's by a relative error of at most 0.015.
Values may be sent and summed in bfloat16 or wider, within the bound.
A program may use at most 128 MiB of HBM per device.

```python
import jax
import jax.numpy as jnp
from jax import lax

S = 6144
NRHS = 256
UR = 1536
BLK = 128
NSN0 = 16
NSN1 = 8
NSN2 = 4
NSN3 = 2
SB = 48
UB = 12


def draw_inverse(key, node_total):

    def draw_node(node_index):
        node_key = jax.random.fold_in(key, node_index)
        noise_key, diag_key = jax.random.split(node_key)
        noise = jax.random.normal(noise_key, (S, S), jnp.float32)
        diagonal = jax.random.uniform(diag_key, (S, 1), jnp.float32, 0.5, 1.5)
        row_ids = lax.broadcasted_iota(jnp.int32, (S, S), 0)
        col_ids = lax.broadcasted_iota(jnp.int32, (S, S), 1)
        lower_part = jnp.where(row_ids > col_ids, noise * S ** (-0.5), 0.0)
        return jnp.where(row_ids == col_ids, diagonal, lower_part)
    stacked = lax.map(draw_node, jnp.arange(node_total, dtype=jnp.int32))
    return stacked.reshape(node_total * S, S)


def draw_table(key, node_total):
    key_list = jax.random.split(jax.random.fold_in(key, 7), node_total)

    def draw_row(row_key):
        return jnp.sort(jax.random.permutation(row_key, S // BLK)[:UR // BLK])
    picked = jax.vmap(draw_row)(key_list).astype(jnp.int32)
    picked = picked.at[0, 0].set(0)
    picked = picked.at[0, UR // BLK - 1].set(S // BLK - 1)
    return picked


def draw_inverse_first(key, part):
    return draw_inverse(key, NSN0).astype(jnp.bfloat16)


def draw_inverse_second(key, part):
    return draw_inverse(key, NSN1).astype(jnp.bfloat16)


def draw_inverse_third(key, part):
    return draw_inverse(key, NSN2).astype(jnp.bfloat16)


def draw_inverse_fourth(key, part):
    return draw_inverse(key, NSN3).astype(jnp.bfloat16)


def draw_blocks_first(key, part):
    return draw_table(key, NSN0)


def draw_blocks_second(key, part):
    return draw_table(key, NSN1)


def draw_blocks_third(key, part):
    return draw_table(key, NSN2)


def level_of(own_key, dims, cuts, least, high):
    def one(position, shards_of):
        draws = jax.random.uniform(jax.random.fold_in(jax.random.fold_in(own_key, 6), position), (shards_of,), jnp.float32, least / len(cuts), high / len(cuts))
        return jnp.repeat(jnp.exp(draws), dims[position] // shards_of).reshape((-1,) + (1,) * (len(dims) - position - 1))

    loudness = one(*cuts[0])
    for cut in cuts[1:]:
        loudness = loudness * one(*cut)
    return loudness


def scatter_about(key, shape, width, most, shards=(), kind=jnp.bfloat16):
    gain = level_of(key, shape, shards, -0.22, 0.18) if shards else 1.0
    values = jax.random.normal(key, shape, jnp.float32) * width * gain
    return jnp.minimum(jnp.maximum(values, -most), most).astype(kind)


def setup_inputs(seed: int = 0) -> dict:
    key_of = jax.random.split(jax.random.key(seed), 16)
    return {
        "loads_first": scatter_about(key_of[0], (NSN0 * S, NRHS), 1.0, 6.0, ((0, 128),)),
        "loads_second": scatter_about(key_of[1], (NSN1 * S, NRHS), 1.0, 6.0, ((0, 128),)),
        "loads_third": scatter_about(key_of[2], (NSN2 * S, NRHS), 1.0, 6.0, ((0, 128),)),
        "loads_fourth": scatter_about(key_of[3], (NSN3 * S, NRHS), 1.0, 6.0, ((0, 128),)),
        "inverse_first": draw_inverse_first(jax.random.fold_in(key_of[15], 71), 0),
        "inverse_second": draw_inverse_second(jax.random.fold_in(key_of[15], 71), 0),
        "inverse_third": draw_inverse_third(jax.random.fold_in(key_of[15], 71), 0),
        "inverse_fourth": draw_inverse_fourth(jax.random.fold_in(key_of[15], 71), 0),
        "panel_first": scatter_about(key_of[8], (UR, NSN0 * S), S ** -0.5, 0.078125, ((1, 128),)),
        "panel_second": scatter_about(key_of[9], (UR, NSN1 * S), S ** -0.5, 0.078125, ((1, 128),)),
        "panel_third": scatter_about(key_of[10], (UR, NSN2 * S), S ** -0.5, 0.078125, ((1, 128),)),
        "panel_fourth": scatter_about(key_of[11], (UR, NSN3 * S), S ** -0.5, 0.078125, ((1, 128),)),
        "blocks_first": draw_blocks_first(jax.random.fold_in(key_of[15], 71), 0),
        "blocks_second": draw_blocks_second(jax.random.fold_in(key_of[15], 71), 0),
        "blocks_third": draw_blocks_third(jax.random.fold_in(key_of[15], 71), 0),
    }


def place_rows(update, table_row):
    blocks = update.reshape(UB, BLK, NRHS)
    spread = jnp.zeros((SB, BLK, NRHS), jnp.float32).at[table_row].add(blocks)
    return spread.reshape(S, NRHS)


def reference(loads_first, loads_second, loads_third, loads_fourth, inverse_first, inverse_second, inverse_third, inverse_fourth, panel_first, panel_second, panel_third, panel_fourth, blocks_first, blocks_second, blocks_third):
    load_list = [loads_first, loads_second, loads_third, loads_fourth]
    inverse_list = [inverse_first, inverse_second, inverse_third, inverse_fourth]
    panel_list = [panel_first, panel_second, panel_third, panel_fourth]
    table_list = [blocks_first, blocks_second, blocks_third]
    node_counts = [NSN0, NSN1, NSN2, NSN3]
    solved_levels = []
    previous = []
    for level_index in range(4):
        solved_blocks = []
        updates = []
        for node_index in range(node_counts[level_index]):
            load_block = load_list[level_index][node_index * S:(node_index + 1) * S]
            if level_index == 0:
                prepared = load_block
            else:
                row_table = table_list[level_index - 1]
                assembled = load_block.astype(jnp.float32) - place_rows(previous[2 * node_index], row_table[2 * node_index]) - place_rows(previous[2 * node_index + 1], row_table[2 * node_index + 1])
                prepared = assembled.astype(jnp.bfloat16)
            inverse_block = inverse_list[level_index][node_index * S:(node_index + 1) * S]
            solved = jnp.dot(inverse_block, prepared, preferred_element_type=jnp.float32).astype(jnp.bfloat16)
            solved_blocks.append(solved)
            panel_block = panel_list[level_index][:, node_index * S:(node_index + 1) * S]
            updates.append(jnp.dot(panel_block, solved, preferred_element_type=jnp.float32))
        solved_levels.append(jnp.concatenate(solved_blocks, 0))
        previous = updates
    ancestor_update = jnp.concatenate(previous, 0)
    return (solved_levels[0], solved_levels[1], solved_levels[2], solved_levels[3], ancestor_update)
```

```python
import jax
import jax.numpy as jnp
from jax import lax
from jax.experimental import pallas as pl
from jax.experimental.pallas import tpu as pltpu
from jax.sharding import PartitionSpec as P

S = 6144
N = 256
UR = 1536
BLK = 128
UB = 12
SB = S // BLK
HALF = 128
ROWS = (768, 384, 192, 96)
MESH = pl.DeviceIdType.MESH
F32 = jnp.float32
BF16 = jnp.bfloat16

DIM = {"y1": (0, 0, 1), "y3": (0, 0, 3), "z1": (0, 1, 0), "z3": (0, 3, 0), "x1": (1, 0, 0)}

REDUCE = (
    (("y1", "y3"), ("y3", "y1")),
    (("y1", "y3", "z1"), ("z1", "y1", "y3")),
    (("y1", "y3", "z1", "z3"), ("z1", "z3", "y1", "y3")),
    (("y1", "y3", "z1", "z3", "x1"), ("z1", "z3", "y1", "y3", "x1")),
)
SIBLING = ("z1", "z3", "x1")

GATHER = {
    1: (("y1", "y3", "z1"), ("z1", "y1", "y3")),
    2: (("y1", "y3", "z1", "z3"), ("z1", "z3", "y1", "y3")),
    3: (("y1", "y3", "z1", "z3", "x1"), ("x1", "z1", "z3", "y1", "y3")),
}
NX = {1: 1, 2: 1, 3: 2}
NZ = {1: 2, 2: 4, 3: 4}
NCH = 2
PCH = 4


def flip(value, mask):
    if mask == 0:
        return value
    if mask == 1:
        return value + 1 - 2 * (value % 2)
    if mask == 2:
        return (value + 2) % 4
    return 3 - value


def bit_of(name, x, z, y):
    if name == "y1":
        return ((y + 1) // 2) % 2
    if name == "y3":
        return y // 2
    if name == "z1":
        return ((z + 1) // 2) % 2
    if name == "z3":
        return z // 2
    return x % 2


def xor(a, b):
    return tuple(i ^ j for i, j in zip(a, b))


def held_before(order, step):
    held = [(0, 0, 0)]
    for name in order[:step]:
        held = held + [xor(h, DIM[name]) for h in held]
    return held


def mask_id(mask):
    return mask[0] * 16 + mask[1] * 4 + mask[2]


class Counter:
    def __init__(self):
        self.used = 0

    def take(self, count=1):
        first = self.used
        self.used += count
        return first


N_SEM = 560
N_LOCAL = 32


def kernel(*refs):
    loads = refs[0:4]
    inverse = refs[4:8]
    panel = refs[8:12]
    tables = (None,) + tuple(refs[12:15])
    outs = refs[15:19]
    out_anc = refs[19]
    scratch = list(refs[20:])

    def pop(count):
        taken = scratch[:count]
        del scratch[:count]
        return taken

    inv = pop(4)
    pan = pop(4)
    first = pop(1)[0]
    lbuf = [None] + pop(3)
    ubuf = pop(3)
    solved = pop(4)
    acc0 = pop(1)[0]
    acc_l = [None] + pop(3)
    cols = [None] + pop(3)
    part, acc = pop(2)
    dsend = pop(4)
    drecv = pop(4)
    stage = [pop(len(REDUCE[k][0])) for k in range(4)]
    arrived = [pop(len(REDUCE[k][0])) for k in range(4)]
    fin_send, fin_recv, anc = pop(3)
    ssem, rsem, lsem = pop(3)

    leaf = lax.axis_index("leaf")
    rows = lax.axis_index("rows")
    x, z, y, c = leaf // 4, leaf % 4, rows // 2, rows % 2
    counter = Counter()
    local = Counter()
    sent = []

    def dev(mask, other_core=False):
        core = 1 - c if other_core else c
        return (flip(x, mask[0]) * 4 + flip(z, mask[1]), flip(y, mask[2]) * 2 + core)

    def by_core(zero, one):
        return tuple(a + c * (b - a) for a, b in zip(zero, one))

    sib = dev((0, 0, 0), True)

    def send(src, dst, si, ri, device):
        pltpu.make_async_remote_copy(
            src_ref=src, dst_ref=dst, send_sem=ssem.at[si], recv_sem=rsem.at[ri],
            device_id=device, device_id_type=MESH,
        ).start()

    def wait_recv(dst, ri):
        pltpu.make_async_remote_copy(
            src_ref=dst, dst_ref=dst, send_sem=ssem.at[0], recv_sem=rsem.at[ri],
            device_id=sib, device_id_type=MESH,
        ).wait_recv()

    def wait_send(src, si):
        pltpu.make_async_remote_copy(
            src_ref=src, dst_ref=src, send_sem=ssem.at[si], recv_sem=rsem.at[0],
            device_id=sib, device_id_type=MESH,
        ).wait_send()

    def fetch(src, dst):
        copy = pltpu.make_async_copy(src, dst, lsem.at[local.take()])
        copy.start()
        return copy

    def fetch_blocks(k):
        sem = lsem.at[local.take()]
        for t in range(SB):
            pltpu.make_async_copy(
                inverse[k].at[:, t * BLK:(t + 1) * BLK], inv[k].at[t], sem
            ).start()
        return pltpu.make_async_copy(inv[k], inv[k], sem)

    barrier = pltpu.get_barrier_semaphore()
    partners = [sib] + [dev(DIM[name]) for name in ("y1", "y3", "z1", "z3", "x1")]
    for partner in partners:
        pl.semaphore_signal(barrier, inc=1, device_id=partner, device_id_type=MESH)
    pl.semaphore_wait(barrier, len(partners))

    ch_rows = ROWS[0] // NCH
    g_recv = {m: counter.take(NCH) for m in (1, 2, 3)}
    g_fwd = {m: counter.take(NCH) for m in (0, 1, 2, 3)}
    g_send = {m: counter.take(NCH) for m in (1, 2, 3)}
    g_fsend = {m: counter.take(NCH) for m in (0, 1, 2, 3)}

    def first_at(mask, ch, core):
        return first.at[flip(y, mask), core, pl.ds(ch * ch_rows, ch_rows)]

    for ch in range(NCH):
        src = loads[0].at[pl.ds(ch * ch_rows, ch_rows)]
        for m in (1, 3):
            send(src, first_at(0, ch, c), g_send[m] + ch, g_recv[m] + ch, dev((0, 0, m)))
            sent.append((src, g_send[m] + ch))
    for ch in range(NCH):
        src = loads[0].at[pl.ds(ch * ch_rows, ch_rows)]
        send(src, first_at(0, ch, c), g_fsend[0] + ch, g_fwd[0] + ch, sib)
        sent.append((src, g_fsend[0] + ch))
    own_first = fetch(loads[0], first.at[y, c])
    inv_copy = [fetch(inverse[0], inv[0])]
    pan_copy = [fetch(panel[0], pan[0])]

    l_recv = {k: counter.take(32) for k in (1, 2, 3)}
    l_fwd = {k: counter.take(32) for k in (1, 2, 3)}
    l_send = {k: counter.take(32) for k in (1, 2, 3)}
    l_fsend = {k: counter.take(32) for k in (1, 2, 3)}

    def l_at(k, mask, core):
        xi = flip(x, mask[0]) % 2 if k == 3 else 0
        zi = flip(z, mask[1]) % NZ[k]
        return lbuf[k].at[xi, zi, flip(y, mask[2]), core]

    def l_source(k, mask):
        return loads[k] if mask == (0, 0, 0) else l_at(k, mask, c)

    def l_step(k, step):
        for core in (0, 1):
            @pl.when(c == core)
            def _(core=core):
                order = GATHER[k][core]
                if step > 0:
                    l_collect(k, order, step - 1)
                dim = DIM[order[step]]
                for held in held_before(order, step):
                    there = xor(held, dim)
                    send(l_source(k, held), l_at(k, held, c), l_send[k] + mask_id(there),
                         l_recv[k] + mask_id(there), dev(dim))

    def l_collect(k, order, step):
        dim = DIM[order[step]]
        for held in held_before(order, step):
            here = xor(held, dim)
            wait_recv(l_at(k, here, c), l_recv[k] + mask_id(here))
            send(l_at(k, here, c), l_at(k, here, c), l_fsend[k] + mask_id(here),
                 l_fwd[k] + mask_id(here), sib)

    def all_masks(k):
        zs = (0, 1) if k == 1 else (0, 1, 2, 3)
        xs = (0, 1) if k == 3 else (0,)
        return [(xm, zm, ym) for xm in xs for zm in zs for ym in range(4)]

    l_own = {}

    def l_begin(k):
        send(loads[k], l_at(k, (0, 0, 0), c), l_fsend[k], l_fwd[k], sib)
        l_own[k] = fetch(loads[k], l_at(k, (0, 0, 0), c))
        for mask in all_masks(k):
            sent.append((loads[k], l_fsend[k] + mask_id(mask)))
            if mask != (0, 0, 0):
                sent.append((loads[k], l_send[k] + mask_id(mask)))

    def l_finish(k):
        for core in (0, 1):
            @pl.when(c == core)
            def _(core=core):
                order = GATHER[k][core]
                l_collect(k, order, len(order) - 1)
        l_own[k].wait()
        for mask in all_masks(k):
            wait_recv(l_at(k, mask, 1 - c), l_fwd[k] + mask_id(mask))

    def l_product(k):
        inv_copy[k].wait()
        whole = jnp.concatenate([inv[k][t] for t in range(SB)], axis=1)
        acc_l[k][...] = jnp.dot(
            whole, lbuf[k][...].reshape(S, N), preferred_element_type=F32
        )

    def gather_columns(k):
        parent = leaf // (2 ** k)
        for j in range(2):
            for i in range(UB):
                t = tables[k][2 * parent + j, i]
                cols[k][j, :, i * BLK:(i + 1) * BLK] = inv[k][t]

    for k in (1, 2, 3):
        l_begin(k)
        l_step(k, 0)
    for k in (1, 2, 3):
        inv_copy.append(fetch_blocks(k))
        pan_copy.append(fetch(panel[k], pan[k]))

    def multiply(mask, same_core):
        yy = flip(y, mask)
        core = c if same_core else 1 - c
        block = 2 * yy + core
        col = pl.multiple_of(block * ROWS[0], ROWS[0])

        @pl.when(block <= rows)
        def _():
            acc0[...] += jnp.dot(
                inv[0][:, pl.ds(col, ROWS[0])], first[yy, core], preferred_element_type=F32
            )

    def g_take(mask):
        for ch in range(NCH):
            ref = first_at(mask, ch, c)
            wait_recv(ref, g_recv[mask] + ch)
            if mask in (1, 3):
                core, onward = (0, 3) if mask == 1 else (1, 1)

                @pl.when(c == core)
                def _():
                    send(ref, ref, g_send[2] + ch, g_recv[2] + ch, dev((0, 0, onward)))
            send(ref, ref, g_fsend[mask] + ch, g_fwd[mask] + ch, sib)
            sent.append((ref, g_fsend[mask] + ch))
            if mask == 2:
                sent.append((ref, g_send[2] + ch))

    def g_other(mask):
        for ch in range(NCH):
            wait_recv(first_at(mask, ch, 1 - c), g_fwd[mask] + ch)

    acc0[...] = jnp.zeros_like(acc0)
    own_first.wait()
    inv_copy[0].wait()
    multiply(0, True)
    g_other(0)
    multiply(0, False)
    g_take(1)
    g_take(3)
    l_step(1, 1)
    multiply(1, True)
    multiply(3, True)
    g_other(1)
    multiply(1, False)
    g_other(3)
    multiply(3, False)
    g_take(2)
    multiply(2, True)
    g_other(2)
    multiply(2, False)
    solved[0][...] = acc0[...].astype(BF16)
    out_copies = [fetch(solved[0], outs[0])]

    def panel_product(k):
        pan_copy[k].wait()
        base_s, base_r = counter.take(PCH), counter.take(PCH)
        size = UR // PCH
        for i in range(PCH):
            at = pl.ds(i * size, size)
            value = jnp.dot(pan[k][at, :], solved[k][...], preferred_element_type=F32)
            low, high = value[:, :HALF], value[:, HALF:]
            dsend[k][at, :] = jnp.where(c == 0, high, low).astype(BF16)
            send(dsend[k].at[at], drecv[k].at[at], base_s + i, base_r + i, sib)
            sent.append((dsend[k].at[at], base_s + i))
            part[at, :] = jnp.where(c == 0, low, high)
        return base_r

    def add_cores(k, base_r):
        size = UR // PCH
        for i in range(PCH):
            at = pl.ds(i * size, size)
            wait_recv(drecv[k].at[at], base_r + i)
            if k < 3:
                acc[at, :] = part[at, :] + drecv[k][at, :].astype(F32)
        if k == 3:
            unit = UR // 32
            for xi in range(2):
                for zi in range(4):
                    for yi in range(4):
                        pos = []
                        for order in REDUCE[3]:
                            value = 0
                            for name in order:
                                value = 2 * value + bit_of(name, xi, zi, yi)
                            pos.append(value)
                        to = (pos[0] + c * (pos[1] - pos[0])) * unit
                        at = pl.ds((xi * 16 + zi * 4 + yi) * unit, unit)
                        acc[pl.ds(pl.multiple_of(to, unit), unit), :] = (
                            part[at, :] + drecv[3][at, :].astype(F32)
                        )

    def bit_at(names):
        zero, one = (bit_of(name, x, z, y) for name in names)
        return zero + c * (one - zero)

    def dev_at(names):
        return by_core(dev(DIM[names[0]]), dev(DIM[names[1]]))

    def reduce_level(k):
        offset, size = 0, UR
        for i, names in enumerate(zip(*REDUCE[k])):
            size //= 2
            bit = bit_at(names)
            give = pl.multiple_of(offset + (1 - bit) * size, size)
            keep = pl.multiple_of(offset + bit * size, size)
            stage[k][i][...] = acc[pl.ds(give, size), :].astype(BF16)
            si, ri = counter.take(), counter.take()
            send(stage[k][i], arrived[k][i], si, ri, dev_at(names))
            sent.append((stage[k][i], si))
            wait_recv(arrived[k][i], ri)
            acc[pl.ds(keep, size), :] += arrived[k][i][...].astype(F32)
            offset = keep
        return offset, size

    def spread_level(k, offset, size, between):
        own = (leaf // (2 ** k)) % 2
        u = ubuf[k]
        forwards = []

        def forward(ref_of):
            si, ri = counter.take(), counter.take()
            send(ref_of, ref_of, si, ri, sib)
            sent.append((ref_of, si))
            forwards.append((ref_of, ri))

        at = pl.ds(pl.multiple_of(offset, size), size)
        u[own, c, at, :] = acc[at, :].astype(BF16)
        si, ri = counter.take(), counter.take()
        send(u.at[own, c, at], u.at[own, c, at], si, ri, dev(DIM[SIBLING[k]]))
        sent.append((u.at[own, c, at], si))
        wait_recv(u.at[1 - own, c, at], ri)
        forward(u.at[:, c, at])
        pairs = list(zip(*REDUCE[k]))
        for i in reversed(range(len(pairs))):
            bit = bit_at(pairs[i])
            at = pl.ds(pl.multiple_of(offset, size), size)
            other = pl.ds(pl.multiple_of(offset + (1 - 2 * bit) * size, size), size)
            si, ri = counter.take(), counter.take()
            send(u.at[:, c, at], u.at[:, c, at], si, ri, dev_at(pairs[i]))
            sent.append((u.at[:, c, at], si))
            if i == 0:
                between()
            wait_recv(u.at[:, c, other], ri)
            forward(u.at[:, c, other])
            offset = offset - bit * size
            size *= 2
        for ref_of, ri in forwards:
            wait_recv(ref_of, ri)

    def solve(k):
        total = acc_l[k][...]
        for j in range(2):
            rhs = jnp.concatenate([ubuf[k - 1][j, 0], ubuf[k - 1][j, 1]], axis=1)
            total = total - jnp.dot(cols[k][j], rhs, preferred_element_type=F32)
        solved[k][...] = total.astype(BF16)
        out_copies.append(fetch(solved[k], outs[k]))

    def before_last(k):
        def run():
            l_finish(k)
            l_product(k)
            gather_columns(k)
        return run

    for k in range(4):
        base = panel_product(k)
        if k == 0:
            l_step(1, 2)
            l_step(2, 1)
            l_step(3, 1)
        if k == 1:
            l_step(2, 3)
            l_step(3, 3)
        if k == 2:
            l_step(3, 4)
        add_cores(k, base)
        offset, size = reduce_level(k)
        if k == 0:
            l_step(2, 2)
            l_step(3, 2)
        if k < 3:
            spread_level(k, offset, size, before_last(k + 1))
            solve(k + 1)

    own_rows = acc[pl.ds(pl.multiple_of(offset + c * 24, 8), 24), :]
    fin_send[...] = acc[pl.ds(pl.multiple_of(offset + (1 - c) * 24, 8), 24), :]
    si, ri = counter.take(), counter.take()
    send(fin_send, fin_recv, si, ri, sib)
    sent.append((fin_send, si))
    wait_recv(fin_recv, ri)
    other_rows = fin_recv[...]
    anc[:, :HALF] = jnp.where(c == 0, own_rows, other_rows)
    anc[:, HALF:] = jnp.where(c == 0, other_rows, own_rows)
    out_copies.append(fetch(anc, out_anc))
    for src, si in sent:
        wait_send(src, si)
    for copy in out_copies:
        copy.wait()
    assert counter.used <= N_SEM and local.used <= N_LOCAL, (counter.used, local.used)


def per_device(*args):
    vmem = pltpu.VMEM
    scratch = [vmem((ROWS[0], S), BF16)] + [vmem((SB, r, BLK), BF16) for r in ROWS[1:]]
    scratch += [vmem((UR, r), BF16) for r in ROWS]
    scratch += [vmem((4, 2, ROWS[0], N), BF16)]
    scratch += [vmem((NX[k], NZ[k], 4, 2, ROWS[k], N), BF16) for k in (1, 2, 3)]
    scratch += [vmem((2, 2, UR, HALF), BF16) for _ in range(3)]
    scratch += [vmem((r, N), BF16) for r in ROWS]
    scratch += [vmem((ROWS[0], N), F32)]
    scratch += [vmem((ROWS[k], N), F32) for k in (1, 2, 3)]
    scratch += [vmem((2, ROWS[k], UR), BF16) for k in (1, 2, 3)]
    scratch += [vmem((UR, HALF), F32)] * 2
    scratch += [vmem((UR, HALF), BF16)] * 8
    for _ in range(2):
        for k in range(4):
            scratch += [vmem((UR >> (i + 1), HALF), BF16) for i in range(len(REDUCE[k][0]))]
    scratch += [vmem((24, HALF), F32), vmem((24, HALF), F32), vmem((24, N), F32)]
    scratch += [
        pltpu.SemaphoreType.DMA((N_SEM,)),
        pltpu.SemaphoreType.DMA((N_SEM,)),
        pltpu.SemaphoreType.DMA((N_LOCAL,)),
    ]
    anywhere = pl.BlockSpec(memory_space=pl.ANY)
    return pl.pallas_call(
        kernel,
        out_shape=tuple(jax.ShapeDtypeStruct((r, N), BF16) for r in ROWS)
        + (jax.ShapeDtypeStruct((24, N), F32),),
        in_specs=[anywhere] * 12 + [pl.BlockSpec(memory_space=pltpu.SMEM)] * 3,
        out_specs=(anywhere,) * 5,
        scratch_shapes=scratch,
        compiler_params=pltpu.CompilerParams(
            collective_id=0, has_side_effects=True, vmem_limit_bytes=63 * 1024 * 1024
        ),
    )(*args)


def solution(mesh):
    split = P(("leaf", "rows"), None)
    in_specs = (split,) * 8 + (P(None, ("leaf", "rows")),) * 4 + (P(),) * 3
    return jax.shard_map(
        per_device, mesh=mesh, in_specs=in_specs, out_specs=(split,) * 5, check_vma=False
    )
```

```python
import jax
import jax.numpy as jnp
from jax import lax
from jax.experimental import pallas as pl
from jax.experimental.pallas import tpu as pltpu
from jax.sharding import PartitionSpec as P

S = 6144
N = 256
UR = 1536
BLK = 128
UB = 12
SB = S // BLK
HALF = 128
ROWS = (768, 384, 192, 96)
MESH = pl.DeviceIdType.MESH
F32 = jnp.float32
BF16 = jnp.bfloat16

STAGE = {
    "y": ((0, 0, 2), (0, 0, 1), (0, 0, 3)),
    "z1": ((0, 1, 0),),
    "z3": ((0, 3, 0),),
    "x1": ((1, 0, 0),),
}

CHIPS = (4, 8, 16, 32)

GATHER = {1: ("y", "z1"), 2: ("y", "z1", "z3"), 3: ("y", "z3", "z1", "x1")}
Y_MASKS = STAGE["y"]
Z_MASKS = ((0, 2, 0), (0, 1, 0), (0, 3, 0))
SPREAD = (
    ((((0, 1, 0),), Y_MASKS), (Y_MASKS, ((0, 1, 0),))),
    ((Z_MASKS, Y_MASKS), (Y_MASKS, Z_MASKS)),
    (
        (tuple((1,) + m[1:] for m in Z_MASKS) + Z_MASKS + ((1, 0, 0),), Y_MASKS),
        (tuple((1,) + m[1:] for m in Y_MASKS) + Y_MASKS + ((1, 0, 0),), Z_MASKS),
    ),
)
NX = {1: 1, 2: 1, 3: 2}
NZ = {1: 2, 2: 4, 3: 4}
NCH = 3
PCH = 4


def flip(value, mask):
    if mask == 0:
        return value
    if mask == 1:
        return value + 1 - 2 * (value % 2)
    if mask == 2:
        return (value + 2) % 4
    return 3 - value


def xor(a, b):
    return tuple(i ^ j for i, j in zip(a, b))


def held_before(order, step):
    held = [(0, 0, 0)]
    for name in order[:step]:
        held = held + [xor(h, m) for m in STAGE[name] for h in held]
    return held


def mask_id(mask):
    return mask[0] * 16 + mask[1] * 4 + mask[2]


class Counter:
    def __init__(self):
        self.used = 0

    def take(self, count=1):
        first = self.used
        self.used += count
        return first


N_SEND = 48
N_RECV = 96
N_LOCAL = 32


def kernel(*refs):
    loads = refs[0:4]
    inverse = refs[4:8]
    panel = refs[8:12]
    tables = (None,) + tuple(refs[12:15])
    outs = refs[15:19]
    out_anc = refs[19]
    scratch = list(refs[20:])

    def pop(count):
        taken = scratch[:count]
        del scratch[:count]
        return taken

    inv = pop(4)
    pan = pop(4)
    first = pop(1)[0]
    lbuf = [None] + pop(3)
    ubuf = pop(3)
    solved = pop(4)
    acc0 = pop(1)[0]
    acc_l = [None] + pop(3)
    cols = [None] + pop(3)
    part = pop(1)[0]
    dsend = pop(4)
    drecv = pop(4)
    stage = pop(4)
    arrived = pop(4)
    pan_t = [None, None] + pop(2)
    fin_acc, fin_send, fin_recv, anc = pop(4)
    ssem, rsem, lsem = pop(3)

    leaf = lax.axis_index("leaf")
    rows = lax.axis_index("rows")
    x, z, y, c = leaf // 4, leaf % 4, rows // 2, rows % 2
    out_sem = Counter()
    in_sem = Counter()
    local = Counter()
    sent = []

    def dev(mask, other_core=False):
        core = 1 - c if other_core else c
        return (flip(x, mask[0]) * 4 + flip(z, mask[1]), flip(y, mask[2]) * 2 + core)

    sib = dev((0, 0, 0), True)

    def send(src, dst, si, ri, device):
        pltpu.make_async_remote_copy(
            src_ref=src, dst_ref=dst, send_sem=ssem.at[si], recv_sem=rsem.at[ri],
            device_id=device, device_id_type=MESH,
        ).start()

    def wait_recv(dst, ri):
        pltpu.make_async_remote_copy(
            src_ref=dst, dst_ref=dst, send_sem=ssem.at[0], recv_sem=rsem.at[ri],
            device_id=sib, device_id_type=MESH,
        ).wait_recv()

    def wait_send(src, si):
        pltpu.make_async_remote_copy(
            src_ref=src, dst_ref=src, send_sem=ssem.at[si], recv_sem=rsem.at[0],
            device_id=sib, device_id_type=MESH,
        ).wait_send()

    def fetch(src, dst):
        copy = pltpu.make_async_copy(src, dst, lsem.at[local.take()])
        copy.start()
        return copy

    def fetch_blocks(k):
        sem = lsem.at[local.take()]
        for t in range(SB):
            pltpu.make_async_copy(
                inverse[k].at[:, t * BLK:(t + 1) * BLK], inv[k].at[t], sem
            ).start()
        return pltpu.make_async_copy(inv[k], inv[k], sem)

    barrier = pltpu.get_barrier_semaphore()
    partners = [sib] + [
        dev((xm, zm, ym))
        for xm in range(2) for zm in range(4) for ym in range(4) if (xm, zm, ym) != (0, 0, 0)
    ]
    for partner in partners:
        pl.semaphore_signal(barrier, inc=1, device_id=partner, device_id_type=MESH)
    pl.semaphore_wait(barrier, len(partners))

    ch_rows = ROWS[0] // NCH
    g_recv = {m: in_sem.take(NCH) for m in (1, 2, 3)}
    g_fwd = {m: in_sem.take() for m in (0, 1, 2, 3)}
    g_send = {m: out_sem.take() for m in (1, 3)}
    g_relay = {m: out_sem.take() for m in (1, 3)}
    g_fsend = {m: out_sem.take() for m in (0, 1, 2, 3)}

    def first_at(mask, ch, core):
        return first.at[flip(y, mask), core, pl.ds(ch * ch_rows, ch_rows)]

    def below(mask):
        return flip(y, mask) < y

    def passes_on(core, block):
        return (c == core) & (block < flip(block, 2))

    l_recv = {k: in_sem.take(len(GATHER[k])) for k in (1, 2, 3)}
    l_fwd = {k: in_sem.take() for k in (1, 2, 3)}
    l_send = {k: out_sem.take(len(GATHER[k])) for k in (1, 2, 3)}
    l_fsend = {k: out_sem.take() for k in (1, 2, 3)}

    def l_bulk(k, step):
        ref = lbuf[k]
        count = len(STAGE[GATHER[k][step]]) * len(held_before(GATHER[k], step))
        if count == 3:
            return ref.at[0, 0, 0:3, 0]
        if count == 4:
            return ref.at[0, 0, :, 0]
        if count == 8:
            return ref.at[0, 0:2, :, 0]
        return ref.at[0, :, :, 0]

    def l_at(k, mask, core):
        xi = flip(x, mask[0]) % 2 if k == 3 else 0
        zi = flip(z, mask[1]) % NZ[k]
        return lbuf[k].at[xi, zi, flip(y, mask[2]), core]

    def l_source(k, mask):
        return loads[k] if mask == (0, 0, 0) else l_at(k, mask, c)

    def l_step(k, step):
        if step > 0:
            l_collect(k, step - 1)
        for mask in STAGE[GATHER[k][step]]:
            for held in held_before(GATHER[k], step):
                send(l_source(k, held), l_at(k, held, c), l_send[k] + step, l_recv[k] + step,
                     dev(mask))
        sent.append((l_bulk(k, step), l_send[k] + step, None))

    def l_collect(k, step):
        wait_recv(l_bulk(k, step), l_recv[k] + step)
        for mask in STAGE[GATHER[k][step]]:
            for held in held_before(GATHER[k], step):
                ref = l_at(k, xor(held, mask), c)
                send(ref, ref, l_fsend[k], l_fwd[k], sib)

    l_own = {}

    def l_begin(k):
        own = l_at(k, (0, 0, 0), c)
        send(loads[k], own, l_fsend[k], l_fwd[k], sib)
        l_own[k] = fetch(loads[k], own)
        sent.append((lbuf[k].at[:, :, :, 0], l_fsend[k], None))

    def l_finish(k):
        l_collect(k, len(GATHER[k]) - 1)
        l_own[k].wait()
        wait_recv(lbuf[k].at[:, :, :, 1 - c], l_fwd[k])

    def l_product(k):
        inv_copy[k].wait()
        whole = jnp.concatenate([inv[k][t] for t in range(SB)], axis=1)
        acc_l[k][...] = jnp.dot(
            whole, lbuf[k][...].reshape(S, N), preferred_element_type=F32
        )

    def gather_columns(k):
        parent = leaf // (2 ** k)
        for j in range(2):
            for i in range(UB):
                t = tables[k][2 * parent + j, i]
                at = j * UR + i * BLK
                cols[k][:, at:at + BLK] = inv[k][t]

    l_step(1, 0)
    for m, core in ((1, 0), (3, 1)):
        wanted = (y < flip(y, m)) | passes_on(core, y)

        @pl.when(wanted)
        def _():
            for ch in range(NCH):
                src = loads[0].at[pl.ds(ch * ch_rows, ch_rows)]
                send(src, first_at(0, ch, c), g_send[m], g_recv[m] + ch, dev((0, 0, m)))

        sent.append((loads[0], g_send[m], wanted))

    @pl.when(c == 0)
    def _():
        send(loads[0], first.at[y, c], g_fsend[0], g_fwd[0], sib)

    sent.append((loads[0], g_fsend[0], c == 0))
    own_first = fetch(loads[0], first.at[y, c])
    inv_copy = [fetch(inverse[0], inv[0])]
    pan_copy = [fetch(panel[0], pan[0])]
    for k in (1, 2, 3):
        l_begin(k)
        inv_copy.append(fetch_blocks(k))
        pan_copy.append(fetch(panel[k], pan[k] if k == 1 else pan_t[k]))

    def multiply(mask, same_core):
        yy = flip(y, mask)
        core = c if same_core else 1 - c
        col = pl.multiple_of((2 * yy + core) * ROWS[0], ROWS[0])
        acc0[...] += jnp.dot(
            inv[0][:, pl.ds(col, ROWS[0])], first[yy, core], preferred_element_type=F32
        )

    def g_take(mask):
        needed = below(mask)
        block = flip(y, mask)
        core, onward = (0, 3) if mask == 1 else (1, 1)
        relayed = passes_on(core, block) if mask != 2 else False

        for ch in range(NCH):
            ref = first_at(mask, ch, c)

            @pl.when(needed | relayed)
            def _():
                wait_recv(ref, g_recv[mask] + ch)

            if mask != 2:
                @pl.when(relayed)
                def _():
                    send(ref, ref, g_relay[mask], g_recv[2] + ch, dev((0, 0, onward)))

            @pl.when(needed)
            def _():
                send(ref, ref, g_fsend[mask], g_fwd[mask], sib)

        if mask != 2:
            sent.append((loads[0], g_relay[mask], relayed))
        sent.append((loads[0], g_fsend[mask], needed))

    def g_multiply(mask):
        @pl.when(below(mask))
        def _():
            multiply(mask, True)
            wait_recv(first.at[flip(y, mask), 1 - c], g_fwd[mask])
            multiply(mask, False)

    acc0[...] = jnp.zeros_like(acc0)
    own_first.wait()
    inv_copy[0].wait()
    multiply(0, True)

    @pl.when(c == 1)
    def _():
        wait_recv(first.at[y, 1 - c], g_fwd[0])
        multiply(0, False)

    l_step(1, 1)
    g_take(1)
    g_take(3)
    l_step(2, 0)
    l_step(3, 0)
    g_multiply(1)
    g_multiply(3)
    g_take(2)
    g_multiply(2)
    solved[0][...] = acc0[...].astype(BF16)
    out_copies = [fetch(solved[0], outs[0])]

    def place_of(k):
        return ((x % 2) * 16 + z * 4 + y) % CHIPS[k]

    def chip_of(k, place):
        whole = (x % 2) * 16 + z * 4 + y
        at = whole - whole % CHIPS[k] + place
        return ((x - x % 2 + at // 16) * 4 + (at // 4) % 4, (at % 4) * 2 + c)

    def update_level(k, between):
        chips, me = CHIPS[k], place_of(k)
        size = UR // chips
        if k < 2:
            pan_copy[k].wait()
        base_d, base_r = in_sem.take(PCH), in_sem.take()
        give_d, give_r = out_sem.take(), out_sem.take()
        rows_of = UR // PCH

        def finish(i):
            at = pl.ds(i * rows_of, rows_of)
            wait_recv(drecv[k].at[at], base_d + i)
            stage[k][at, :] = (part[at, :] + drecv[k][at, :].astype(F32)).astype(BF16)
            for q in range(i * chips // PCH, (i + 1) * chips // PCH):
                @pl.when(q != me)
                def _():
                    send(stage[k].at[pl.ds(q * size, size)], arrived[k].at[me],
                         give_r, base_r, chip_of(k, q))

        for i in range(PCH):
            at = pl.ds(i * rows_of, rows_of)
            value = jnp.dot(pan[k][at, :], solved[k][...], preferred_element_type=F32)
            low, high = value[:, :HALF], value[:, HALF:]
            dsend[k][at, :] = jnp.where(c == 0, high, low).astype(BF16)
            send(dsend[k].at[at], drecv[k].at[at], give_d, base_d + i, sib)
            part[at, :] = jnp.where(c == 0, low, high)
        for i in range(PCH):
            finish(i)
        between()
        mine = pl.ds(pl.multiple_of(me * size, size), size)
        total = part[mine, :] + drecv[k][mine, :].astype(F32)
        wait_recv(arrived[k].at[0:chips - 1], base_r)
        for i in range(1, chips):
            total = total + arrived[k][(me + i) % chips].astype(F32)
        sent.append((dsend[k], give_d, None))
        sent.append((arrived[k].at[0:chips - 1], give_r, None))
        return total

    def spread_level(k, total, between):
        chips = 2 * CHIPS[k]
        size = UR // CHIPS[k]
        u = ubuf[k]
        most = max(len(near) for near, _ in SPREAD[k])
        base_a, base_b, base_f = in_sem.take(most), in_sem.take(3), in_sem.take()
        give, give_f = out_sem.take(), out_sem.take()

        def piece(mask):
            at = (flip(x, mask[0]) % 2) * 16 + flip(z, mask[1]) * 4 + flip(y, mask[2])
            at = at % chips * size
            return u.at[c, pl.ds(pl.multiple_of(at, size), size)]

        def across(ref):
            send(ref, ref, give_f, base_f, sib)

        own = piece((0, 0, 0))
        own[...] = total.astype(BF16)
        for core, (near, far) in enumerate(SPREAD[k]):
            @pl.when(c == core)
            def _():
                for i, m in enumerate(near):
                    send(own, own, give, base_a + i, dev(m))
                for i, m in enumerate(far):
                    send(own, own, give, base_b + i, dev(m))
                across(own)
                for i in reversed(range(len(near))):
                    ref = piece(near[i])
                    wait_recv(ref, base_a + i)
                    for j, m in enumerate(far):
                        send(ref, ref, give, base_b + j, dev(m))
                    across(ref)

        between()
        for core, (near, far) in enumerate(SPREAD[k]):
            @pl.when(c == core)
            def _():
                for j in reversed(range(len(far))):
                    wait_recv(u.at[c, 0:(len(near) + 1) * size], base_b + j)
                    for m in ((0, 0, 0),) + near:
                        across(piece(xor(m, far[j])))

        sent.append((u.at[c, 0:(chips - 1) * size], give, None))
        sent.append((u.at[c], give_f, None))
        wait_recv(u.at[1 - c], base_f)
        rhs = jnp.concatenate([u[0], u[1]], axis=1)
        value = acc_l[k + 1][...] - jnp.dot(cols[k + 1][...], rhs, preferred_element_type=F32)
        solved[k + 1][...] = value.astype(BF16)
        out_copies.append(fetch(solved[k + 1], outs[k + 1]))

    def in_reduce(k):
        def run():
            if k == 0:
                for j in (2, 3):
                    pan_copy[j].wait()
                    pan[j][...] = pan_t[j][...].T
                l_step(3, 1)
                l_step(2, 1)
            if k == 1:
                l_step(3, 2)
        return run

    def in_spread(k):
        def run():
            if k == 0:
                l_step(2, 2)
            if k == 1:
                l_step(3, 3)
            l_finish(k + 1)
            l_product(k + 1)
            gather_columns(k + 1)
        return run

    for k in range(4):
        total = update_level(k, in_reduce(k))
        if k < 3:
            spread_level(k, total, in_spread(k))

    fin_acc[...] = total
    own_rows = fin_acc[pl.ds(pl.multiple_of(c * 24, 8), 24), :]
    fin_send[...] = fin_acc[pl.ds(pl.multiple_of((1 - c) * 24, 8), 24), :]
    si, ri = out_sem.take(), in_sem.take()
    send(fin_send, fin_recv, si, ri, sib)
    sent.append((fin_send, si, None))
    wait_recv(fin_recv, ri)
    other_rows = fin_recv[...]
    anc[:, :HALF] = jnp.where(c == 0, own_rows, other_rows)
    anc[:, HALF:] = jnp.where(c == 0, other_rows, own_rows)
    out_copies.append(fetch(anc, out_anc))
    for src, si, cond in sent:
        if cond is None:
            wait_send(src, si)
        else:
            pl.when(cond)(lambda src=src, si=si: wait_send(src, si))
    for copy in out_copies:
        copy.wait()
    used = (out_sem.used, in_sem.used, local.used)
    assert used <= (N_SEND, N_RECV, N_LOCAL) and max(used) <= N_RECV, used


def hand_over(*refs):
    given, taken, held, sem = refs[:5], refs[5:10], refs[10:15], refs[15]
    ins = [pltpu.make_async_copy(a, b, sem.at[i]) for i, (a, b) in enumerate(zip(given, held))]
    outs = [pltpu.make_async_copy(a, b, sem.at[5 + i]) for i, (a, b) in enumerate(zip(held, taken))]
    for copy in ins:
        copy.start()
    for first, second in zip(ins, outs):
        first.wait()
        second.start()
    for copy in outs:
        copy.wait()


def per_device(*args):
    vmem = pltpu.VMEM
    scratch = [vmem((ROWS[0], S), BF16)] + [vmem((SB, r, BLK), BF16) for r in ROWS[1:]]
    scratch += [vmem((UR, r), BF16) for r in ROWS]
    scratch += [vmem((4, 2, ROWS[0], N), BF16)]
    scratch += [vmem((NX[k], NZ[k], 4, 2, ROWS[k], N), BF16) for k in (1, 2, 3)]
    scratch += [vmem((2, 2 * UR, HALF), BF16) for _ in range(3)]
    scratch += [vmem((r, N), BF16) for r in ROWS]
    scratch += [vmem((ROWS[0], N), F32)]
    scratch += [vmem((ROWS[k], N), F32) for k in (1, 2, 3)]
    scratch += [vmem((ROWS[k], 2 * UR), BF16) for k in (1, 2, 3)]
    scratch += [vmem((UR, HALF), F32)]
    scratch += [vmem((UR, HALF), BF16)] * 12
    scratch += [vmem((n, UR // n, HALF), BF16) for n in CHIPS]
    scratch += [vmem((ROWS[k], UR), BF16) for k in (2, 3)]
    scratch += [vmem((48, HALF), F32), vmem((24, HALF), F32), vmem((24, HALF), F32), vmem((24, N), F32)]
    scratch += [
        pltpu.SemaphoreType.DMA((N_SEND,)),
        pltpu.SemaphoreType.DMA((N_RECV,)),
        pltpu.SemaphoreType.DMA((N_LOCAL,)),
    ]
    anywhere = pl.BlockSpec(memory_space=pl.ANY)
    shapes = tuple(jax.ShapeDtypeStruct((r, N), BF16) for r in ROWS)
    shapes += (jax.ShapeDtypeStruct((24, N), F32),)
    args = args[:10] + (args[10].T, args[11].T) + args[12:]
    results = pl.pallas_call(
        kernel,
        out_shape=shapes,
        in_specs=[anywhere] * 12 + [pl.BlockSpec(memory_space=pltpu.SMEM)] * 3,
        out_specs=(anywhere,) * 5,
        scratch_shapes=scratch,
        compiler_params=pltpu.CompilerParams(
            collective_id=0, has_side_effects=True, vmem_limit_bytes=63 * 1024 * 1024
        ),
    )(*args)
    return pl.pallas_call(
        hand_over,
        out_shape=shapes,
        in_specs=[anywhere] * 5,
        out_specs=(anywhere,) * 5,
        scratch_shapes=[vmem(a.shape, a.dtype) for a in shapes] + [pltpu.SemaphoreType.DMA((10,))],
    )(*results)


def solution(mesh):
    split = P(("leaf", "rows"), None)
    in_specs = (split,) * 8 + (P(None, ("leaf", "rows")),) * 4 + (P(),) * 3
    return jax.shard_map(
        per_device, mesh=mesh, in_specs=in_specs, out_specs=(split,) * 5, check_vma=False
    )
```

```python
import jax
import jax.numpy as jnp
from jax import lax
from jax.experimental import pallas as pl
from jax.experimental.pallas import tpu as pltpu
from jax.sharding import PartitionSpec as P

S = 6144
N = 256
UR = 1536
BLK = 128
UB = 12
SB = S // BLK
HALF = 128
ROWS = (768, 384, 192, 96)
MESH = pl.DeviceIdType.MESH
F32 = jnp.float32
BF16 = jnp.bfloat16

STAGE = {
    "y": ((0, 0, 2), (0, 0, 1), (0, 0, 3)),
    "z1": ((0, 1, 0),),
    "z3": ((0, 3, 0),),
    "x1": ((1, 0, 0),),
}

CHIPS = (4, 8, 16, 32)

GATHER = {1: ("y", "z1"), 2: ("y", "z1", "z3"), 3: ("y", "z3", "z1", "x1")}
Y_MASKS = STAGE["y"]
Z_MASKS = ((0, 2, 0), (0, 1, 0), (0, 3, 0))
SPREAD = (
    ((((0, 1, 0),), Y_MASKS), (Y_MASKS, ((0, 1, 0),))),
    ((Z_MASKS, Y_MASKS), (Y_MASKS, Z_MASKS)),
    (
        (tuple((1,) + m[1:] for m in Z_MASKS) + Z_MASKS + ((1, 0, 0),), Y_MASKS),
        (tuple((1,) + m[1:] for m in Y_MASKS) + Y_MASKS + ((1, 0, 0),), Z_MASKS),
    ),
)
NX = {1: 1, 2: 1, 3: 2}
NZ = {1: 2, 2: 4, 3: 4}
NCH = 3
PCH = 4


def flip(value, mask):
    if mask == 0:
        return value
    if mask == 1:
        return value + 1 - 2 * (value % 2)
    if mask == 2:
        return (value + 2) % 4
    return 3 - value


def xor(a, b):
    return tuple(i ^ j for i, j in zip(a, b))


def held_before(order, step):
    held = [(0, 0, 0)]
    for name in order[:step]:
        held = held + [xor(h, m) for m in STAGE[name] for h in held]
    return held


def mask_id(mask):
    return mask[0] * 16 + mask[1] * 4 + mask[2]


class Counter:
    def __init__(self):
        self.used = 0

    def take(self, count=1):
        first = self.used
        self.used += count
        return first


N_SEND = 48
N_RECV = 96
N_LOCAL = 32


def kernel(*refs):
    loads = refs[0:4]
    inverse = refs[4:8]
    panel = refs[8:12]
    tables = (None,) + tuple(refs[12:15])
    outs = refs[15:19]
    out_anc = refs[19]
    scratch = list(refs[20:])

    def pop(count):
        taken = scratch[:count]
        del scratch[:count]
        return taken

    inv = pop(4)
    pan = pop(4)
    first = pop(1)[0]
    lbuf = [None] + pop(3)
    ubuf = pop(3)
    solved = pop(4)
    acc0 = pop(1)[0]
    acc_l = [None] + pop(3)
    cols = [None] + pop(3)
    part = pop(1)[0]
    dsend = pop(4)
    drecv = pop(4)
    stage = pop(4)
    arrived = pop(4)
    pan_t = [None, None] + pop(2)
    fin_acc, fin_send, fin_recv, anc = pop(4)
    ssem, rsem, lsem = pop(3)

    leaf = lax.axis_index("leaf")
    rows = lax.axis_index("rows")
    x, z, y, c = leaf // 4, leaf % 4, rows // 2, rows % 2
    out_sem = Counter()
    in_sem = Counter()
    local = Counter()
    sent = []

    def dev(mask, other_core=False):
        core = 1 - c if other_core else c
        return (flip(x, mask[0]) * 4 + flip(z, mask[1]), flip(y, mask[2]) * 2 + core)

    sib = dev((0, 0, 0), True)

    def send(src, dst, si, ri, device):
        pltpu.make_async_remote_copy(
            src_ref=src, dst_ref=dst, send_sem=ssem.at[si], recv_sem=rsem.at[ri],
            device_id=device, device_id_type=MESH,
        ).start()

    def wait_recv(dst, ri):
        pltpu.make_async_remote_copy(
            src_ref=dst, dst_ref=dst, send_sem=ssem.at[0], recv_sem=rsem.at[ri],
            device_id=sib, device_id_type=MESH,
        ).wait_recv()

    def wait_send(src, si):
        pltpu.make_async_remote_copy(
            src_ref=src, dst_ref=src, send_sem=ssem.at[si], recv_sem=rsem.at[0],
            device_id=sib, device_id_type=MESH,
        ).wait_send()

    def fetch(src, dst):
        copy = pltpu.make_async_copy(src, dst, lsem.at[local.take()])
        copy.start()
        return copy

    def fetch_blocks(k):
        sem = lsem.at[local.take()]
        for t in range(SB):
            pltpu.make_async_copy(
                inverse[k].at[:, t * BLK:(t + 1) * BLK], inv[k].at[t], sem
            ).start()
        return pltpu.make_async_copy(inv[k], inv[k], sem)

    barrier = pltpu.get_barrier_semaphore()
    hops = (0, 1, 2, 1)
    others = [(xm, zm, ym) for xm in range(2) for zm in range(4) for ym in range(4)][1:]
    others.sort(key=lambda m: -(m[0] + hops[m[1]] + hops[m[2]]))
    partners = [dev(m) for m in others] + [sib]
    for partner in partners:
        pl.semaphore_signal(barrier, inc=1, device_id=partner, device_id_type=MESH)
    pl.semaphore_wait(barrier, len(partners))

    ch_rows = ROWS[0] // NCH
    g_recv = {m: in_sem.take(NCH) for m in (1, 2, 3)}
    g_fwd = {m: in_sem.take() for m in (0, 1, 2, 3)}
    g_send = {m: out_sem.take() for m in (1, 3)}
    g_relay = {m: out_sem.take() for m in (1, 3)}
    g_fsend = {m: out_sem.take() for m in (0, 1, 2, 3)}

    def first_at(mask, ch, core):
        return first.at[flip(y, mask), core, pl.ds(ch * ch_rows, ch_rows)]

    def below(mask):
        return flip(y, mask) < y

    def passes_on(core, block):
        return (c == core) & (block < flip(block, 2))

    l_recv = {k: in_sem.take(len(GATHER[k])) for k in (1, 2, 3)}
    l_fwd = {k: in_sem.take() for k in (1, 2, 3)}
    l_send = {k: out_sem.take(len(GATHER[k])) for k in (1, 2, 3)}
    l_fsend = {k: out_sem.take() for k in (1, 2, 3)}

    def l_bulk(k, step):
        ref = lbuf[k]
        count = len(STAGE[GATHER[k][step]]) * len(held_before(GATHER[k], step))
        if count == 3:
            return ref.at[0, 0, 0:3, 0]
        if count == 4:
            return ref.at[0, 0, :, 0]
        if count == 8:
            return ref.at[0, 0:2, :, 0]
        return ref.at[0, :, :, 0]

    def l_at(k, mask, core):
        xi = flip(x, mask[0]) % 2 if k == 3 else 0
        zi = flip(z, mask[1]) % NZ[k]
        return lbuf[k].at[xi, zi, flip(y, mask[2]), core]

    def l_source(k, mask):
        return loads[k] if mask == (0, 0, 0) else l_at(k, mask, c)

    def l_step(k, step):
        if step > 0:
            l_collect(k, step - 1)
        for mask in STAGE[GATHER[k][step]]:
            for held in held_before(GATHER[k], step):
                send(l_source(k, held), l_at(k, held, c), l_send[k] + step, l_recv[k] + step,
                     dev(mask))
        sent.append((l_bulk(k, step), l_send[k] + step, None))

    def l_collect(k, step):
        wait_recv(l_bulk(k, step), l_recv[k] + step)
        for mask in STAGE[GATHER[k][step]]:
            for held in held_before(GATHER[k], step):
                ref = l_at(k, xor(held, mask), c)
                send(ref, ref, l_fsend[k], l_fwd[k], sib)

    l_own = {}

    def l_begin(k):
        own = l_at(k, (0, 0, 0), c)
        send(loads[k], own, l_fsend[k], l_fwd[k], sib)
        l_own[k] = fetch(loads[k], own)
        sent.append((lbuf[k].at[:, :, :, 0], l_fsend[k], None))

    def l_finish(k):
        l_own[k].wait()
        wait_recv(lbuf[k].at[:, :, :, 1 - c], l_fwd[k])

    def l_product(k):
        whole = jnp.concatenate([inv[k][t] for t in range(SB)], axis=1)
        acc_l[k][...] = jnp.dot(
            whole, lbuf[k][...].reshape(S, N), preferred_element_type=F32
        )

    def gather_columns(k):
        inv_copy[k].wait()
        parent = leaf // (2 ** k)
        for j in range(2):
            for i in range(UB):
                t = tables[k][2 * parent + j, i]
                at = j * UR + i * BLK
                cols[k][:, at:at + BLK] = inv[k][t]

    l_step(1, 0)
    for m, core in ((1, 0), (3, 1)):
        wanted = (y < flip(y, m)) | passes_on(core, y)

        @pl.when(wanted)
        def _():
            for ch in range(NCH):
                src = loads[0].at[pl.ds(ch * ch_rows, ch_rows)]
                send(src, first_at(0, ch, c), g_send[m], g_recv[m] + ch, dev((0, 0, m)))

        sent.append((loads[0], g_send[m], wanted))

    @pl.when(c == 0)
    def _():
        send(loads[0], first.at[y, c], g_fsend[0], g_fwd[0], sib)

    sent.append((loads[0], g_fsend[0], c == 0))
    own_first = fetch(loads[0], first.at[y, c])
    inv_copy = [fetch(inverse[0], inv[0])]
    pan_copy = [fetch(panel[0], pan[0])]
    for k in (1, 2, 3):
        l_begin(k)
        inv_copy.append(fetch_blocks(k))
        pan_copy.append(fetch(panel[k], pan[k] if k == 1 else pan_t[k]))

    def multiply(mask, same_core):
        yy = flip(y, mask)
        core = c if same_core else 1 - c
        col = pl.multiple_of((2 * yy + core) * ROWS[0], ROWS[0])
        acc0[...] += jnp.dot(
            inv[0][:, pl.ds(col, ROWS[0])], first[yy, core], preferred_element_type=F32
        )

    def g_take(mask, ch):
        needed = below(mask)
        block = flip(y, mask)
        core, onward = (0, 3) if mask == 1 else (1, 1)
        ref = first_at(mask, ch, c)
        relayed = passes_on(core, block) if mask != 2 else False

        @pl.when(needed | relayed)
        def _():
            wait_recv(ref, g_recv[mask] + ch)

        if mask != 2:
            @pl.when(relayed)
            def _():
                send(ref, ref, g_relay[mask], g_recv[2] + ch, dev((0, 0, onward)))

        @pl.when(needed)
        def _():
            send(ref, ref, g_fsend[mask], g_fwd[mask], sib)

        if ch == 0:
            if mask != 2:
                sent.append((loads[0], g_relay[mask], relayed))
            sent.append((loads[0], g_fsend[mask], needed))

    def g_multiply(mask):
        @pl.when(below(mask))
        def _():
            multiply(mask, True)
            wait_recv(first.at[flip(y, mask), 1 - c], g_fwd[mask])
            multiply(mask, False)

    acc0[...] = jnp.zeros_like(acc0)
    own_first.wait()
    inv_copy[0].wait()
    multiply(0, True)

    @pl.when(c == 1)
    def _():
        wait_recv(first.at[y, 1 - c], g_fwd[0])
        multiply(0, False)

    l_step(1, 1)
    for ch in range(NCH):
        g_take(1, ch)
        g_take(3, ch)
    l_step(2, 0)
    l_step(3, 0)
    g_multiply(1)
    g_multiply(3)
    for ch in range(NCH):
        g_take(2, ch)
    g_multiply(2)
    solved[0][...] = acc0[...].astype(BF16)
    out_copies = [fetch(solved[0], outs[0])]

    def place_of(k):
        return ((x % 2) * 16 + z * 4 + y) % CHIPS[k]

    def chip_of(k, place):
        whole = (x % 2) * 16 + z * 4 + y
        at = whole - whole % CHIPS[k] + place
        return ((x - x % 2 + at // 16) * 4 + (at // 4) % 4, (at % 4) * 2 + c)

    def update_level(k, between):
        chips, me = CHIPS[k], place_of(k)
        size = UR // chips
        if k < 2:
            pan_copy[k].wait()
        base_d, base_r = in_sem.take(PCH), in_sem.take()
        give_d, give_r = out_sem.take(), out_sem.take()
        rows_of = UR // PCH

        def finish(i):
            at = pl.ds(i * rows_of, rows_of)
            wait_recv(drecv[k].at[at], base_d + i)
            stage[k][at, :] = (part[at, :] + drecv[k][at, :].astype(F32)).astype(BF16)
            for q in range(i * chips // PCH, (i + 1) * chips // PCH):
                @pl.when(q != me)
                def _():
                    send(stage[k].at[pl.ds(q * size, size)], arrived[k].at[me],
                         give_r, base_r, chip_of(k, q))

        for i in range(PCH):
            at = pl.ds(i * rows_of, rows_of)
            value = jnp.dot(pan[k][at, :], solved[k][...], preferred_element_type=F32)
            low, high = value[:, :HALF], value[:, HALF:]
            dsend[k][at, :] = jnp.where(c == 0, high, low).astype(BF16)
            send(dsend[k].at[at], drecv[k].at[at], give_d, base_d + i, sib)
            part[at, :] = jnp.where(c == 0, low, high)
        for i in range(PCH):
            finish(i)
        between()
        mine = pl.ds(pl.multiple_of(me * size, size), size)
        total = part[mine, :] + drecv[k][mine, :].astype(F32)
        wait_recv(arrived[k].at[0:chips - 1], base_r)
        for i in range(1, chips):
            total = total + arrived[k][(me + i) % chips].astype(F32)
        sent.append((dsend[k], give_d, None))
        sent.append((arrived[k].at[0:chips - 1], give_r, None))
        return total

    def spread_level(k, total, between):
        chips = 2 * CHIPS[k]
        size = UR // CHIPS[k]
        u = ubuf[k]
        most = max(len(near) for near, _ in SPREAD[k])
        base_a, base_b, base_f = in_sem.take(most), in_sem.take(3), in_sem.take()
        give, give_f = out_sem.take(), out_sem.take()

        def piece(mask):
            at = (flip(x, mask[0]) % 2) * 16 + flip(z, mask[1]) * 4 + flip(y, mask[2])
            at = at % chips * size
            return u.at[c, pl.ds(pl.multiple_of(at, size), size)]

        def across(ref):
            send(ref, ref, give_f, base_f, sib)

        own = piece((0, 0, 0))
        own[...] = total.astype(BF16)
        for core, (near, far) in enumerate(SPREAD[k]):
            @pl.when(c == core)
            def _():
                for i, m in enumerate(near):
                    send(own, own, give, base_a + i, dev(m))
                for i, m in enumerate(far):
                    send(own, own, give, base_b + i, dev(m))
                across(own)
                for i in reversed(range(len(near))):
                    ref = piece(near[i])
                    wait_recv(ref, base_a + i)
                    for j, m in enumerate(far):
                        send(ref, ref, give, base_b + j, dev(m))
                    across(ref)

        between()
        for core, (near, far) in enumerate(SPREAD[k]):
            @pl.when(c == core)
            def _():
                for j in reversed(range(len(far))):
                    wait_recv(u.at[c, 0:(len(near) + 1) * size], base_b + j)
                    for m in ((0, 0, 0),) + near:
                        across(piece(xor(m, far[j])))

        sent.append((u.at[c, 0:(chips - 1) * size], give, None))
        sent.append((u.at[c], give_f, None))
        wait_recv(u.at[1 - c], base_f)
        rhs = jnp.concatenate([u[0], u[1]], axis=1)
        value = acc_l[k + 1][...] - jnp.dot(cols[k + 1][...], rhs, preferred_element_type=F32)
        solved[k + 1][...] = value.astype(BF16)
        out_copies.append(fetch(solved[k + 1], outs[k + 1]))

    def in_reduce(k):
        def run():
            if k == 0:
                for j in (2, 3):
                    pan_copy[j].wait()
                    pan[j][...] = pan_t[j][...].T
                l_collect(1, 1)
            if k == 1:
                l_step(3, 3)
            if k < 3:
                gather_columns(k + 1)
        return run

    def in_spread(k):
        def run():
            if k == 0:
                l_step(2, 2)
                l_step(3, 2)
            else:
                l_collect(k + 1, len(GATHER[k + 1]) - 1)
            l_finish(k + 1)
            l_product(k + 1)
        return run

    l_step(2, 1)
    l_step(3, 1)
    for k in range(4):
        total = update_level(k, in_reduce(k))
        if k < 3:
            spread_level(k, total, in_spread(k))

    fin_acc[...] = total
    own_rows = fin_acc[pl.ds(pl.multiple_of(c * 24, 8), 24), :]
    fin_send[...] = fin_acc[pl.ds(pl.multiple_of((1 - c) * 24, 8), 24), :]
    si, ri = out_sem.take(), in_sem.take()
    send(fin_send, fin_recv, si, ri, sib)
    sent.append((fin_send, si, None))
    wait_recv(fin_recv, ri)
    other_rows = fin_recv[...]
    anc[:, :HALF] = jnp.where(c == 0, own_rows, other_rows)
    anc[:, HALF:] = jnp.where(c == 0, other_rows, own_rows)
    out_copies.append(fetch(anc, out_anc))
    for src, si, cond in sent:
        if cond is None:
            wait_send(src, si)
        else:
            pl.when(cond)(lambda src=src, si=si: wait_send(src, si))
    for copy in out_copies:
        copy.wait()
    used = (out_sem.used, in_sem.used, local.used)
    assert used <= (N_SEND, N_RECV, N_LOCAL) and max(used) <= N_RECV, used


def hand_over(*refs):
    given, taken, held, sem = refs[:5], refs[5:10], refs[10:15], refs[15]
    ins = [pltpu.make_async_copy(a, b, sem.at[i]) for i, (a, b) in enumerate(zip(given, held))]
    outs = [pltpu.make_async_copy(a, b, sem.at[5 + i]) for i, (a, b) in enumerate(zip(held, taken))]
    for copy in ins:
        copy.start()
    for first, second in zip(ins, outs):
        first.wait()
        second.start()
    for copy in outs:
        copy.wait()


def per_device(*args):
    vmem = pltpu.VMEM
    scratch = [vmem((ROWS[0], S), BF16)] + [vmem((SB, r, BLK), BF16) for r in ROWS[1:]]
    scratch += [vmem((UR, r), BF16) for r in ROWS]
    scratch += [vmem((4, 2, ROWS[0], N), BF16)]
    scratch += [vmem((NX[k], NZ[k], 4, 2, ROWS[k], N), BF16) for k in (1, 2, 3)]
    scratch += [vmem((2, 2 * UR, HALF), BF16) for _ in range(3)]
    scratch += [vmem((r, N), BF16) for r in ROWS]
    scratch += [vmem((ROWS[0], N), F32)]
    scratch += [vmem((ROWS[k], N), F32) for k in (1, 2, 3)]
    scratch += [vmem((ROWS[k], 2 * UR), BF16) for k in (1, 2, 3)]
    scratch += [vmem((UR, HALF), F32)]
    scratch += [vmem((UR, HALF), BF16)] * 12
    scratch += [vmem((n, UR // n, HALF), BF16) for n in CHIPS]
    scratch += [vmem((ROWS[k], UR), BF16) for k in (2, 3)]
    scratch += [vmem((48, HALF), F32), vmem((24, HALF), F32), vmem((24, HALF), F32), vmem((24, N), F32)]
    scratch += [
        pltpu.SemaphoreType.DMA((N_SEND,)),
        pltpu.SemaphoreType.DMA((N_RECV,)),
        pltpu.SemaphoreType.DMA((N_LOCAL,)),
    ]
    anywhere = pl.BlockSpec(memory_space=pl.ANY)
    shapes = tuple(jax.ShapeDtypeStruct((r, N), BF16) for r in ROWS)
    shapes += (jax.ShapeDtypeStruct((24, N), F32),)
    args = args[:10] + (args[10].T, args[11].T) + args[12:]
    results = pl.pallas_call(
        kernel,
        out_shape=shapes,
        in_specs=[anywhere] * 12 + [pl.BlockSpec(memory_space=pltpu.SMEM)] * 3,
        out_specs=(anywhere,) * 5,
        scratch_shapes=scratch,
        compiler_params=pltpu.CompilerParams(
            collective_id=0, has_side_effects=True, vmem_limit_bytes=63 * 1024 * 1024
        ),
    )(*args)
    return pl.pallas_call(
        hand_over,
        out_shape=shapes,
        in_specs=[anywhere] * 5,
        out_specs=(anywhere,) * 5,
        scratch_shapes=[vmem(a.shape, a.dtype) for a in shapes] + [pltpu.SemaphoreType.DMA((10,))],
    )(*results)


def solution(mesh):
    split = P(("leaf", "rows"), None)
    in_specs = (split,) * 8 + (P(None, ("leaf", "rows")),) * 4 + (P(),) * 3
    return jax.shard_map(
        per_device, mesh=mesh, in_specs=in_specs, out_specs=(split,) * 5, check_vma=False
    )
```

```python
import jax
import jax.numpy as jnp
from jax import lax
from jax.experimental import pallas as pl
from jax.experimental.pallas import tpu as pltpu
from jax.sharding import PartitionSpec as P

S = 6144
N = 256
UR = 1536
BLK = 128
UB = 12
SB = S // BLK
HALF = 128
ROWS = (768, 384, 192, 96)
MESH = pl.DeviceIdType.MESH
F32 = jnp.float32
BF16 = jnp.bfloat16

STAGE = {
    "y": ((0, 0, 2), (0, 0, 1), (0, 0, 3)),
    "z1": ((0, 1, 0),),
    "z3": ((0, 3, 0),),
    "x1": ((1, 0, 0),),
}

CHIPS = (4, 8, 16, 32)

GATHER = {1: ("y", "z1"), 2: ("y", "z1", "z3"), 3: ("y", "z3", "z1", "x1")}
Y_MASKS = STAGE["y"]
Z_MASKS = ((0, 2, 0), (0, 1, 0), (0, 3, 0))
SPREAD = (
    ((((0, 1, 0),), Y_MASKS), (Y_MASKS, ((0, 1, 0),))),
    ((Z_MASKS, Y_MASKS), (Y_MASKS, Z_MASKS)),
    (
        (tuple((1,) + m[1:] for m in Z_MASKS) + Z_MASKS + ((1, 0, 0),), Y_MASKS),
        (tuple((1,) + m[1:] for m in Y_MASKS) + Y_MASKS + ((1, 0, 0),), Z_MASKS),
    ),
)
NX = {1: 1, 2: 1, 3: 2}
NZ = {1: 2, 2: 4, 3: 4}
NCH = 3
PCH = 4
PARTS = (2, 2, 2, 1)


def flip(value, mask):
    if mask == 0:
        return value
    if mask == 1:
        return value + 1 - 2 * (value % 2)
    if mask == 2:
        return (value + 2) % 4
    return 3 - value


def xor(a, b):
    return tuple(i ^ j for i, j in zip(a, b))


def held_before(order, step):
    held = [(0, 0, 0)]
    for name in order[:step]:
        held = held + [xor(h, m) for m in STAGE[name] for h in held]
    return held


def mask_id(mask):
    return mask[0] * 16 + mask[1] * 4 + mask[2]


class Counter:
    def __init__(self):
        self.used = 0

    def take(self, count=1):
        first = self.used
        self.used += count
        return first


N_SEND = 48
N_RECV = 112
N_LOCAL = 32


def kernel(*refs):
    loads = refs[0:4]
    inverse = refs[4:8]
    panel = refs[8:12]
    tables = (None,) + tuple(refs[12:15])
    outs = refs[15:19]
    out_anc = refs[19]
    scratch = list(refs[20:])

    def pop(count):
        taken = scratch[:count]
        del scratch[:count]
        return taken

    inv = pop(4)
    pan = pop(4)
    first = pop(1)[0]
    lbuf = [None] + pop(3)
    ubuf = pop(3)
    solved = pop(4)
    acc0 = pop(1)[0]
    acc_l = [None] + pop(3)
    cols = [None] + pop(3)
    part = pop(1)[0]
    dsend = pop(4)
    drecv = pop(4)
    stage = pop(4)
    arrived = pop(4)
    pan_t = [None, None] + pop(2)
    fin_acc, fin_send, fin_recv, anc = pop(4)
    ssem, rsem, lsem = pop(3)

    leaf = lax.axis_index("leaf")
    rows = lax.axis_index("rows")
    x, z, y, c = leaf // 4, leaf % 4, rows // 2, rows % 2
    out_sem = Counter()
    in_sem = Counter()
    local = Counter()
    sent = []

    def dev(mask, other_core=False):
        core = 1 - c if other_core else c
        return (flip(x, mask[0]) * 4 + flip(z, mask[1]), flip(y, mask[2]) * 2 + core)

    sib = dev((0, 0, 0), True)

    def send(src, dst, si, ri, device):
        pltpu.make_async_remote_copy(
            src_ref=src, dst_ref=dst, send_sem=ssem.at[si], recv_sem=rsem.at[ri],
            device_id=device, device_id_type=MESH,
        ).start()

    def wait_recv(dst, ri):
        pltpu.make_async_remote_copy(
            src_ref=dst, dst_ref=dst, send_sem=ssem.at[0], recv_sem=rsem.at[ri],
            device_id=sib, device_id_type=MESH,
        ).wait_recv()

    def wait_send(src, si):
        pltpu.make_async_remote_copy(
            src_ref=src, dst_ref=src, send_sem=ssem.at[si], recv_sem=rsem.at[0],
            device_id=sib, device_id_type=MESH,
        ).wait_send()

    def fetch(src, dst):
        copy = pltpu.make_async_copy(src, dst, lsem.at[local.take()])
        copy.start()
        return copy

    def fetch_blocks(k):
        sem = lsem.at[local.take()]
        for t in range(SB):
            pltpu.make_async_copy(
                inverse[k].at[:, t * BLK:(t + 1) * BLK], inv[k].at[t], sem
            ).start()
        return pltpu.make_async_copy(inv[k], inv[k], sem)

    barrier = pltpu.get_barrier_semaphore()
    hops = (0, 1, 2, 1)
    others = [(xm, zm, ym) for xm in range(2) for zm in range(4) for ym in range(4)][1:]
    others.sort(key=lambda m: -(m[0] + hops[m[1]] + hops[m[2]]))
    partners = [dev(m) for m in others] + [sib]
    for partner in partners:
        pl.semaphore_signal(barrier, inc=1, device_id=partner, device_id_type=MESH)
    own_first = fetch(loads[0], first.at[y, c])
    inv_copy = [fetch(inverse[0], inv[0])]
    pan_copy = [fetch(panel[0], pan[0])]
    for k in (1, 2, 3):
        inv_copy.append(fetch_blocks(k))
        pan_copy.append(fetch(panel[k], pan[k] if k == 1 else pan_t[k]))
    pl.semaphore_wait(barrier, len(partners))

    ch_rows = ROWS[0] // NCH
    g_recv = {m: in_sem.take(NCH) for m in (1, 2, 3)}
    g_fwd = {m: in_sem.take() for m in (0, 1, 2, 3)}
    g_send = {m: out_sem.take() for m in (1, 3)}
    g_relay = {m: out_sem.take() for m in (1, 3)}
    g_fsend = {m: out_sem.take() for m in (0, 1, 2, 3)}

    def first_at(mask, ch, core):
        return first.at[flip(y, mask), core, pl.ds(ch * ch_rows, ch_rows)]

    def below(mask):
        return flip(y, mask) < y

    def passes_on(core, block):
        return (c == core) & (block < flip(block, 2))

    l_recv = {k: in_sem.take(len(GATHER[k])) for k in (1, 2, 3)}
    l_fwd = {k: in_sem.take() for k in (1, 2, 3)}
    l_send = {k: out_sem.take(len(GATHER[k])) for k in (1, 2, 3)}
    l_fsend = {k: out_sem.take() for k in (1, 2, 3)}

    def l_bulk(k, step):
        ref = lbuf[k]
        count = len(STAGE[GATHER[k][step]]) * len(held_before(GATHER[k], step))
        if count == 3:
            return ref.at[0, 0, 0:3, 0]
        if count == 4:
            return ref.at[0, 0, :, 0]
        if count == 8:
            return ref.at[0, 0:2, :, 0]
        return ref.at[0, :, :, 0]

    def l_at(k, mask, core):
        xi = flip(x, mask[0]) % 2 if k == 3 else 0
        zi = flip(z, mask[1]) % NZ[k]
        return lbuf[k].at[xi, zi, flip(y, mask[2]), core]

    def l_source(k, mask):
        return loads[k] if mask == (0, 0, 0) else l_at(k, mask, c)

    def l_step(k, step, cond=None):
        def run():
            if step > 0:
                l_collect(k, step - 1)
            for mask in STAGE[GATHER[k][step]]:
                for held in held_before(GATHER[k], step):
                    send(l_source(k, held), l_at(k, held, c), l_send[k] + step, l_recv[k] + step,
                         dev(mask))

        if cond is None:
            run()
        else:
            pl.when(cond)(run)
        if (k, step) not in l_done:
            sent.append((l_bulk(k, step), l_send[k] + step, None))
        l_done.add((k, step))

    def l_collect(k, step):
        wait_recv(l_bulk(k, step), l_recv[k] + step)
        for mask in STAGE[GATHER[k][step]]:
            for held in held_before(GATHER[k], step):
                ref = l_at(k, xor(held, mask), c)
                send(ref, ref, l_fsend[k], l_fwd[k], sib)

    l_own = {}
    l_done = set()

    def l_begin(k):
        own = l_at(k, (0, 0, 0), c)
        send(loads[k], own, l_fsend[k], l_fwd[k], sib)
        l_own[k] = fetch(loads[k], own)
        sent.append((lbuf[k].at[:, :, :, 0], l_fsend[k], None))

    def l_finish(k):
        l_own[k].wait()
        wait_recv(lbuf[k].at[:, :, :, 1 - c], l_fwd[k])

    def l_product(k):
        whole = jnp.concatenate([inv[k][t] for t in range(SB)], axis=1)
        acc_l[k][...] = jnp.dot(
            whole, lbuf[k][...].reshape(S, N), preferred_element_type=F32
        )

    def gather_columns(k):
        inv_copy[k].wait()
        parent = leaf // (2 ** k)
        for j in range(2):
            for i in range(UB):
                t = tables[k][2 * parent + j, i]
                at = j * UR + i * BLK
                cols[k][:, at:at + BLK] = inv[k][t]

    l_step(1, 0)
    for m, core in ((1, 0), (3, 1)):
        wanted = (y < flip(y, m)) | passes_on(core, y)

        @pl.when(wanted)
        def _():
            for ch in range(NCH):
                src = loads[0].at[pl.ds(ch * ch_rows, ch_rows)]
                send(src, first_at(0, ch, c), g_send[m], g_recv[m] + ch, dev((0, 0, m)))

        sent.append((loads[0], g_send[m], wanted))

    @pl.when(c == 0)
    def _():
        send(loads[0], first.at[y, c], g_fsend[0], g_fwd[0], sib)

    sent.append((loads[0], g_fsend[0], c == 0))
    for k in (1, 2, 3):
        l_begin(k)

    def multiply(mask, same_core):
        yy = flip(y, mask)
        core = c if same_core else 1 - c
        col = pl.multiple_of((2 * yy + core) * ROWS[0], ROWS[0])
        acc0[...] += jnp.dot(
            inv[0][:, pl.ds(col, ROWS[0])], first[yy, core], preferred_element_type=F32
        )

    def g_take(mask, ch):
        needed = below(mask)
        block = flip(y, mask)
        core, onward = (0, 3) if mask == 1 else (1, 1)
        ref = first_at(mask, ch, c)
        relayed = passes_on(core, block) if mask != 2 else False

        @pl.when(needed | relayed)
        def _():
            wait_recv(ref, g_recv[mask] + ch)

        if mask != 2:
            @pl.when(relayed)
            def _():
                send(ref, ref, g_relay[mask], g_recv[2] + ch, dev((0, 0, onward)))

        @pl.when(needed)
        def _():
            send(ref, ref, g_fsend[mask], g_fwd[mask], sib)

        if ch == 0:
            if mask != 2:
                sent.append((loads[0], g_relay[mask], relayed))
            sent.append((loads[0], g_fsend[mask], needed))

    def g_multiply(mask):
        @pl.when(below(mask))
        def _():
            multiply(mask, True)
            wait_recv(first.at[flip(y, mask), 1 - c], g_fwd[mask])
            multiply(mask, False)

    acc0[...] = jnp.zeros_like(acc0)
    own_first.wait()
    inv_copy[0].wait()
    multiply(0, True)

    @pl.when(c == 1)
    def _():
        wait_recv(first.at[y, 1 - c], g_fwd[0])
        multiply(0, False)

    l_step(1, 1)
    for ch in range(NCH):
        g_take(1, ch)
        g_take(3, ch)
    l_step(2, 0)
    l_step(3, 0)
    g_multiply(1)
    g_multiply(3)
    for ch in range(NCH):
        g_take(2, ch)
    g_multiply(2)
    solved[0][...] = acc0[...].astype(BF16)
    out_copies = [fetch(solved[0], outs[0])]

    def place_of(k):
        return ((x % 2) * 16 + z * 4 + y) % CHIPS[k]

    def chip_of(k, place):
        whole = (x % 2) * 16 + z * 4 + y
        at = whole - whole % CHIPS[k] + place
        return ((x - x % 2 + at // 16) * 4 + (at // 4) % 4, (at % 4) * 2 + c)

    def update_level(k, between):
        chips, me = CHIPS[k], place_of(k)
        size = UR // chips
        if k < 2:
            pan_copy[k].wait()
        parts = PARTS[k]
        part_size = size // parts
        base_d, base_r = in_sem.take(PCH), in_sem.take(parts)
        give_d, give_r = out_sem.take(), out_sem.take()
        rows_of = UR // PCH

        def finish(i):
            at = pl.ds(i * rows_of, rows_of)
            wait_recv(drecv[k].at[at], base_d + i)
            stage[k][at, :] = (part[at, :] + drecv[k][at, :].astype(F32)).astype(BF16)
            for q in range(i * chips // PCH, (i + 1) * chips // PCH):
                give_piece(q, 0)

        def give_piece(q, h):
            @pl.when(q != me)
            def _():
                send(stage[k].at[pl.ds(q * size + h * part_size, part_size)],
                     arrived[k].at[h, me], give_r, base_r + h, chip_of(k, q))

        for i in range(PCH):
            at = pl.ds(i * rows_of, rows_of)
            value = jnp.dot(pan[k][at, :], solved[k][...], preferred_element_type=F32)
            low, high = value[:, :HALF], value[:, HALF:]
            dsend[k][at, :] = jnp.where(c == 0, high, low).astype(BF16)
            send(dsend[k].at[at], drecv[k].at[at], give_d, base_d + i, sib)
            part[at, :] = jnp.where(c == 0, low, high)
        for i in range(PCH):
            finish(i)
        for h in range(1, parts):
            for q in range(chips):
                give_piece(q, h)
        between()
        sent.append((dsend[k], give_d, None))
        sent.append((arrived[k].at[:, 0:chips - 1], give_r, None))

        def total_of(h):
            at = pl.ds(pl.multiple_of(me * size + h * part_size, part_size), part_size)
            total = part[at, :] + drecv[k][at, :].astype(F32)
            wait_recv(arrived[k].at[h, 0:chips - 1], base_r + h)
            for i in range(1, chips):
                total = total + arrived[k][h, (me + i) % chips].astype(F32)
            return total

        return total_of

    def spread_level(k, total_of, between):
        chips = 2 * CHIPS[k]
        size = UR // CHIPS[k]
        u = ubuf[k]
        most = max(len(near) for near, _ in SPREAD[k])
        parts = PARTS[k]
        part_size = size // parts
        base_a, base_b = in_sem.take(most * parts), in_sem.take(3 * parts)
        base_f = in_sem.take()
        give, give_f = out_sem.take(), out_sem.take()

        def piece(mask, h):
            at = (flip(x, mask[0]) % 2) * 16 + flip(z, mask[1]) * 4 + flip(y, mask[2])
            at = at % chips * size + h * part_size
            return u.at[c, pl.ds(pl.multiple_of(at, part_size), part_size)]

        def across(ref):
            send(ref, ref, give_f, base_f, sib)

        for h in range(parts):
            own = piece((0, 0, 0), h)
            own[...] = total_of(h).astype(BF16)
            for core, (near, far) in enumerate(SPREAD[k]):
                @pl.when(c == core)
                def _():
                    for i, m in enumerate(near):
                        send(own, own, give, base_a + h * most + i, dev(m))
                    for j, m in enumerate(far):
                        send(own, own, give, base_b + h * 3 + j, dev(m))
                    across(own)

        for core, (near, far) in enumerate(SPREAD[k]):
            @pl.when(c == core)
            def _():
                for h in range(parts):
                    for i in reversed(range(len(near))):
                        ref = piece(near[i], h)
                        wait_recv(ref, base_a + h * most + i)
                        for j, m in enumerate(far):
                            send(ref, ref, give, base_b + h * 3 + j, dev(m))
                        across(ref)

        between()
        for core, (near, far) in enumerate(SPREAD[k]):
            @pl.when(c == core)
            def _():
                for h in range(parts):
                    for j in reversed(range(len(far))):
                        wait_recv(u.at[c, 0:(len(near) + 1) * part_size], base_b + h * 3 + j)
                        for m in ((0, 0, 0),) + near:
                            across(piece(xor(m, far[j]), h))

        sent.append((u.at[c, 0:(chips - 1) * size], give, None))
        sent.append((u.at[c], give_f, None))
        wait_recv(u.at[1 - c], base_f)
        rhs = jnp.concatenate([u[0], u[1]], axis=1)
        value = acc_l[k + 1][...] - jnp.dot(cols[k + 1][...], rhs, preferred_element_type=F32)
        solved[k + 1][...] = value.astype(BF16)
        out_copies.append(fetch(solved[k + 1], outs[k + 1]))

    def in_reduce(k):
        def run():
            if k == 0:
                for j in (2, 3):
                    pan_copy[j].wait()
                    pan[j][...] = pan_t[j][...].T
                l_step(2, 1, y == 3)
                l_step(3, 1, y == 3)
                l_collect(1, 1)
            if k == 1:
                l_step(3, 3)
            if k < 3:
                gather_columns(k + 1)
        return run

    def in_spread(k):
        def run():
            if k == 0:
                l_step(2, 2)
                l_step(3, 2)
            else:
                l_collect(k + 1, len(GATHER[k + 1]) - 1)
            l_finish(k + 1)
            l_product(k + 1)
        return run

    l_step(2, 1, y < 3)
    l_step(3, 1, y < 3)
    for k in range(4):
        total_of = update_level(k, in_reduce(k))
        if k < 3:
            spread_level(k, total_of, in_spread(k))

    fin_acc[...] = total_of(0)
    own_rows = fin_acc[pl.ds(pl.multiple_of(c * 24, 8), 24), :]
    fin_send[...] = fin_acc[pl.ds(pl.multiple_of((1 - c) * 24, 8), 24), :]
    si, ri = out_sem.take(), in_sem.take()
    send(fin_send, fin_recv, si, ri, sib)
    sent.append((fin_send, si, None))
    wait_recv(fin_recv, ri)
    other_rows = fin_recv[...]
    anc[:, :HALF] = jnp.where(c == 0, own_rows, other_rows)
    anc[:, HALF:] = jnp.where(c == 0, other_rows, own_rows)
    out_copies.append(fetch(anc, out_anc))
    for src, si, cond in sent:
        if cond is None:
            wait_send(src, si)
        else:
            pl.when(cond)(lambda src=src, si=si: wait_send(src, si))
    for copy in out_copies:
        copy.wait()
    used = (out_sem.used, in_sem.used, local.used)
    assert used <= (N_SEND, N_RECV, N_LOCAL) and max(used) <= N_RECV, used


def hand_over(*refs):
    given, taken, held, sem = refs[:5], refs[5:10], refs[10:15], refs[15]
    ins = [pltpu.make_async_copy(a, b, sem.at[i]) for i, (a, b) in enumerate(zip(given, held))]
    outs = [pltpu.make_async_copy(a, b, sem.at[5 + i]) for i, (a, b) in enumerate(zip(held, taken))]
    for copy in ins:
        copy.start()
    for first, second in zip(ins, outs):
        first.wait()
        second.start()
    for copy in outs:
        copy.wait()


def per_device(*args):
    vmem = pltpu.VMEM
    scratch = [vmem((ROWS[0], S), BF16)] + [vmem((SB, r, BLK), BF16) for r in ROWS[1:]]
    scratch += [vmem((UR, r), BF16) for r in ROWS]
    scratch += [vmem((4, 2, ROWS[0], N), BF16)]
    scratch += [vmem((NX[k], NZ[k], 4, 2, ROWS[k], N), BF16) for k in (1, 2, 3)]
    scratch += [vmem((2, 2 * UR, HALF), BF16) for _ in range(3)]
    scratch += [vmem((r, N), BF16) for r in ROWS]
    scratch += [vmem((ROWS[0], N), F32)]
    scratch += [vmem((ROWS[k], N), F32) for k in (1, 2, 3)]
    scratch += [vmem((ROWS[k], 2 * UR), BF16) for k in (1, 2, 3)]
    scratch += [vmem((UR, HALF), F32)]
    scratch += [vmem((UR, HALF), BF16)] * 12
    scratch += [vmem((p, n, UR // n // p, HALF), BF16) for n, p in zip(CHIPS, PARTS)]
    scratch += [vmem((ROWS[k], UR), BF16) for k in (2, 3)]
    scratch += [vmem((48, HALF), F32), vmem((24, HALF), F32), vmem((24, HALF), F32), vmem((24, N), F32)]
    scratch += [
        pltpu.SemaphoreType.DMA((N_SEND,)),
        pltpu.SemaphoreType.DMA((N_RECV,)),
        pltpu.SemaphoreType.DMA((N_LOCAL,)),
    ]
    anywhere = pl.BlockSpec(memory_space=pl.ANY)
    shapes = tuple(jax.ShapeDtypeStruct((r, N), BF16) for r in ROWS)
    shapes += (jax.ShapeDtypeStruct((24, N), F32),)
    args = args[:10] + (args[10].T, args[11].T) + args[12:]
    results = pl.pallas_call(
        kernel,
        out_shape=shapes,
        in_specs=[anywhere] * 12 + [pl.BlockSpec(memory_space=pltpu.SMEM)] * 3,
        out_specs=(anywhere,) * 5,
        scratch_shapes=scratch,
        compiler_params=pltpu.CompilerParams(
            collective_id=0, has_side_effects=True, vmem_limit_bytes=63 * 1024 * 1024
        ),
    )(*args)
    return pl.pallas_call(
        hand_over,
        out_shape=shapes,
        in_specs=[anywhere] * 5,
        out_specs=(anywhere,) * 5,
        scratch_shapes=[vmem(a.shape, a.dtype) for a in shapes] + [pltpu.SemaphoreType.DMA((10,))],
    )(*results)


def solution(mesh):
    split = P(("leaf", "rows"), None)
    in_specs = (split,) * 8 + (P(None, ("leaf", "rows")),) * 4 + (P(),) * 3
    return jax.shard_map(
        per_device, mesh=mesh, in_specs=in_specs, out_specs=(split,) * 5, check_vma=False
    )
```

```python
import jax
import jax.numpy as jnp
from jax import lax
from jax.experimental import pallas as pl
from jax.experimental.pallas import tpu as pltpu
from jax.sharding import PartitionSpec as P

S = 6144
N = 256
UR = 1536
BLK = 128
UB = 12
SB = S // BLK
HALF = 128
ROWS = (768, 384, 192, 96)
MESH = pl.DeviceIdType.MESH
F32 = jnp.float32
BF16 = jnp.bfloat16

STAGE = {
    "y": ((0, 0, 2), (0, 0, 1), (0, 0, 3)),
    "z1": ((0, 1, 0),),
    "z3": ((0, 3, 0),),
    "x1": ((1, 0, 0),),
}

CHIPS = (4, 8, 16, 32)

GATHER = {
    1: (("y", "z1"), ("y", "z1")),
    2: (("y", "z3", "z1"), ("y", "z1", "z3")),
    3: (("y", "z1", "z3", "x1"), ("y", "z3", "z1", "x1")),
}
Y_MASKS = STAGE["y"]
Z_MASKS = ((0, 2, 0), (0, 1, 0), (0, 3, 0))
SPREAD = (
    ((((0, 1, 0),), Y_MASKS), (Y_MASKS, ((0, 1, 0),))),
    ((Z_MASKS, Y_MASKS), (Y_MASKS, Z_MASKS)),
    (
        (tuple((1,) + m[1:] for m in Z_MASKS) + Z_MASKS + ((1, 0, 0),), Y_MASKS),
        (tuple((1,) + m[1:] for m in Y_MASKS) + Y_MASKS + ((1, 0, 0),), Z_MASKS),
    ),
)
NX = {1: 1, 2: 1, 3: 2}
NZ = {1: 2, 2: 4, 3: 4}
NCH = 3
PCH = 4
PARTS = (2, 2, 2, 1)


def flip(value, mask):
    if mask == 0:
        return value
    if mask == 1:
        return value + 1 - 2 * (value % 2)
    if mask == 2:
        return (value + 2) % 4
    return 3 - value


def xor(a, b):
    return tuple(i ^ j for i, j in zip(a, b))


def held_before(order, step):
    held = [(0, 0, 0)]
    for name in order[:step]:
        held = held + [xor(h, m) for m in STAGE[name] for h in held]
    return held


def mask_id(mask):
    return mask[0] * 16 + mask[1] * 4 + mask[2]


class Counter:
    def __init__(self):
        self.used = 0

    def take(self, count=1):
        first = self.used
        self.used += count
        return first


N_SEND = 35
N_RECV = 96
N_LOCAL = 17


def kernel(*refs):
    loads = refs[0:4]
    inverse = refs[4:8]
    panel = refs[8:12]
    tables = (None,) + tuple(refs[12:15])
    outs = refs[15:19]
    out_anc = refs[19]
    scratch = list(refs[20:])

    def pop(count):
        taken = scratch[:count]
        del scratch[:count]
        return taken

    inv = pop(4)
    pan = pop(4)
    first = pop(1)[0]
    lbuf = [None] + pop(3)
    ubuf = pop(3)
    solved = pop(4)
    acc0 = pop(1)[0]
    acc_l = [None] + pop(3)
    cols = [None] + pop(3)
    part = pop(1)[0]
    dsend = pop(4)
    drecv = pop(4)
    stage = pop(4)
    arrived = pop(4)
    pan_t = [None, None] + pop(2)
    fin_acc, fin_send, fin_recv, anc = pop(4)
    ssem, rsem, lsem = pop(3)

    leaf = lax.axis_index("leaf")
    rows = lax.axis_index("rows")
    x, z, y, c = leaf // 4, leaf % 4, rows // 2, rows % 2
    out_sem = Counter()
    in_sem = Counter()
    local = Counter()
    sent = []

    def dev(mask, other_core=False):
        core = 1 - c if other_core else c
        return (flip(x, mask[0]) * 4 + flip(z, mask[1]), flip(y, mask[2]) * 2 + core)

    sib = dev((0, 0, 0), True)

    def send(src, dst, si, ri, device):
        pltpu.make_async_remote_copy(
            src_ref=src, dst_ref=dst, send_sem=ssem.at[si], recv_sem=rsem.at[ri],
            device_id=device, device_id_type=MESH,
        ).start()

    def wait_recv(dst, ri):
        pltpu.make_async_remote_copy(
            src_ref=dst, dst_ref=dst, send_sem=ssem.at[0], recv_sem=rsem.at[ri],
            device_id=sib, device_id_type=MESH,
        ).wait_recv()

    def wait_send(src, si):
        pltpu.make_async_remote_copy(
            src_ref=src, dst_ref=src, send_sem=ssem.at[si], recv_sem=rsem.at[0],
            device_id=sib, device_id_type=MESH,
        ).wait_send()

    def fetch(src, dst):
        copy = pltpu.make_async_copy(src, dst, lsem.at[local.take()])
        copy.start()
        return copy

    def fetch_blocks(k):
        sem = lsem.at[local.take()]
        for t in range(SB):
            pltpu.make_async_copy(
                inverse[k].at[:, t * BLK:(t + 1) * BLK], inv[k].at[t], sem
            ).start()
        return pltpu.make_async_copy(inv[k], inv[k], sem)

    barrier = pltpu.get_barrier_semaphore()
    hops = (0, 1, 2, 1)
    others = [(xm, zm, ym) for xm in range(2) for zm in range(4) for ym in range(4)][1:]
    others.sort(key=lambda m: -(m[0] + hops[m[1]] + hops[m[2]]))
    partners = [dev(m) for m in others] + [sib]
    for partner in partners:
        pl.semaphore_signal(barrier, inc=1, device_id=partner, device_id_type=MESH)
    own_first = fetch(loads[0], first.at[y, c])
    inv_copy = [fetch(inverse[0], inv[0])]
    pan_copy = [fetch(panel[0], pan[0])]
    for k in (1, 2, 3):
        inv_copy.append(fetch_blocks(k))
        pan_copy.append(fetch(panel[k], pan[k] if k == 1 else pan_t[k]))
    pl.semaphore_wait(barrier, len(partners))

    ch_rows = ROWS[0] // NCH
    g_recv = {m: in_sem.take(NCH) for m in (1, 2, 3)}
    g_fwd = {m: in_sem.take() for m in (0, 1, 2, 3)}
    g_send = {m: out_sem.take() for m in (1, 3)}
    g_relay = {m: out_sem.take() for m in (1, 3)}
    g_fsend = {m: out_sem.take() for m in (0, 1, 2, 3)}

    def first_at(mask, ch, core):
        return first.at[flip(y, mask), core, pl.ds(ch * ch_rows, ch_rows)]

    def below(mask):
        return flip(y, mask) < y

    def passes_on(core, block):
        return (c == core) & (block < flip(block, 2))

    l_recv = {k: in_sem.take(len(GATHER[k][0])) for k in (1, 2, 3)}
    l_fwd = {k: in_sem.take() for k in (1, 2, 3)}
    l_send = {k: out_sem.take(len(GATHER[k][0])) for k in (1, 2, 3)}
    l_fsend = {k: out_sem.take() for k in (1, 2, 3)}

    def l_bulk(k, step):
        ref = lbuf[k]
        order = GATHER[k][0]
        count = len(STAGE[order[step]]) * len(held_before(order, step))
        if count == 3:
            return ref.at[0, 0, 0:3, 0]
        if count == 4:
            return ref.at[0, 0, :, 0]
        if count == 8:
            return ref.at[0, 0:2, :, 0]
        return ref.at[0, :, :, 0]

    def l_at(k, mask, core):
        xi = flip(x, mask[0]) % 2 if k == 3 else 0
        zi = flip(z, mask[1]) % NZ[k]
        return lbuf[k].at[xi, zi, flip(y, mask[2]), core]

    def l_source(k, mask):
        return loads[k] if mask == (0, 0, 0) else l_at(k, mask, c)

    def by_order(k, step, run):
        zero, one = GATHER[k]
        if zero[:step + 1] == one[:step + 1]:
            run(zero)
        else:
            pl.when(c == 0)(lambda: run(zero))
            pl.when(c == 1)(lambda: run(one))

    def l_step(k, step, cond=None):
        def stage_of(order):
            for mask in STAGE[order[step]]:
                for held in held_before(order, step):
                    send(l_source(k, held), l_at(k, held, c), l_send[k] + step, l_recv[k] + step,
                         dev(mask))

        def run():
            if step > 0:
                l_collect(k, step - 1)
            by_order(k, step, stage_of)

        if cond is None:
            run()
        else:
            pl.when(cond)(run)
        if (k, step) not in l_done:
            sent.append((l_bulk(k, step), l_send[k] + step, None))
        l_done.add((k, step))

    def l_collect(k, step):
        wait_recv(l_bulk(k, step), l_recv[k] + step)

        def forward(order):
            for mask in STAGE[order[step]]:
                for held in held_before(order, step):
                    ref = l_at(k, xor(held, mask), c)
                    send(ref, ref, l_fsend[k], l_fwd[k], sib)

        by_order(k, step, forward)

    l_own = {}
    l_done = set()

    def l_begin(k):
        own = l_at(k, (0, 0, 0), c)
        send(loads[k], own, l_fsend[k], l_fwd[k], sib)
        l_own[k] = fetch(loads[k], own)
        sent.append((lbuf[k].at[:, :, :, 0], l_fsend[k], None))

    def l_finish(k):
        l_own[k].wait()
        wait_recv(lbuf[k].at[:, :, :, 1 - c], l_fwd[k])

    def l_product(k):
        whole = jnp.concatenate([inv[k][t] for t in range(SB)], axis=1)
        acc_l[k][...] = jnp.dot(
            whole, lbuf[k][...].reshape(S, N), preferred_element_type=F32
        )

    def gather_columns(k):
        inv_copy[k].wait()
        parent = leaf // (2 ** k)
        for j in range(2):
            for i in range(UB):
                t = tables[k][2 * parent + j, i]
                at = j * UR + i * BLK
                cols[k][:, at:at + BLK] = inv[k][t]

    l_step(1, 0)
    for m, core in ((1, 0), (3, 1)):
        wanted = (y < flip(y, m)) | passes_on(core, y)

        @pl.when(wanted)
        def _():
            for ch in range(NCH):
                src = loads[0].at[pl.ds(ch * ch_rows, ch_rows)]
                send(src, first_at(0, ch, c), g_send[m], g_recv[m] + ch, dev((0, 0, m)))

        sent.append((loads[0], g_send[m], wanted))

    @pl.when(c == 0)
    def _():
        send(loads[0], first.at[y, c], g_fsend[0], g_fwd[0], sib)

    sent.append((loads[0], g_fsend[0], c == 0))
    for k in (1, 2, 3):
        l_begin(k)

    def multiply(mask, same_core):
        yy = flip(y, mask)
        core = c if same_core else 1 - c
        col = pl.multiple_of((2 * yy + core) * ROWS[0], ROWS[0])
        acc0[...] += jnp.dot(
            inv[0][:, pl.ds(col, ROWS[0])], first[yy, core], preferred_element_type=F32
        )

    def g_take(mask, ch):
        needed = below(mask)
        block = flip(y, mask)
        core, onward = (0, 3) if mask == 1 else (1, 1)
        ref = first_at(mask, ch, c)
        relayed = passes_on(core, block) if mask != 2 else False

        @pl.when(needed | relayed)
        def _():
            wait_recv(ref, g_recv[mask] + ch)

        if mask != 2:
            @pl.when(relayed)
            def _():
                send(ref, ref, g_relay[mask], g_recv[2] + ch, dev((0, 0, onward)))

        @pl.when(needed)
        def _():
            send(ref, ref, g_fsend[mask], g_fwd[mask], sib)

        if ch == 0:
            if mask != 2:
                sent.append((loads[0], g_relay[mask], relayed))
            sent.append((loads[0], g_fsend[mask], needed))

    def g_multiply(mask):
        @pl.when(below(mask))
        def _():
            multiply(mask, True)
            wait_recv(first.at[flip(y, mask), 1 - c], g_fwd[mask])
            multiply(mask, False)

    acc0[...] = jnp.zeros_like(acc0)
    own_first.wait()
    inv_copy[0].wait()
    multiply(0, True)

    @pl.when(c == 1)
    def _():
        wait_recv(first.at[y, 1 - c], g_fwd[0])
        multiply(0, False)

    l_step(1, 1)
    for ch in range(NCH):
        g_take(1, ch)
        g_take(3, ch)
    l_step(2, 0)
    l_step(3, 0)
    g_multiply(1)
    g_multiply(3)
    for ch in range(NCH):
        g_take(2, ch)
    g_multiply(2)
    solved[0][...] = acc0[...].astype(BF16)
    out_copies = [fetch(solved[0], outs[0])]

    def place_of(k):
        return ((x % 2) * 16 + z * 4 + y) % CHIPS[k]

    def chip_of(k, place):
        whole = (x % 2) * 16 + z * 4 + y
        at = whole - whole % CHIPS[k] + place
        return ((x - x % 2 + at // 16) * 4 + (at // 4) % 4, (at % 4) * 2 + c)

    def update_level(k, between):
        chips, me = CHIPS[k], place_of(k)
        size = UR // chips
        if k < 2:
            pan_copy[k].wait()
        parts = PARTS[k]
        part_size = size // parts
        base_d, base_r = in_sem.take(PCH), in_sem.take(parts)
        give_d, give_r = out_sem.take(), out_sem.take()
        rows_of = UR // PCH

        def finish(i):
            at = pl.ds(i * rows_of, rows_of)
            wait_recv(drecv[k].at[at], base_d + i)
            stage[k][at, :] = (part[at, :] + drecv[k][at, :].astype(F32)).astype(BF16)
            for q in range(i * chips // PCH, (i + 1) * chips // PCH):
                give_piece(q, 0)

        def give_piece(q, h):
            @pl.when(q != me)
            def _():
                send(stage[k].at[pl.ds(q * size + h * part_size, part_size)],
                     arrived[k].at[h, me], give_r, base_r + h, chip_of(k, q))

        for i in range(PCH):
            at = pl.ds(i * rows_of, rows_of)
            value = jnp.dot(pan[k][at, :], solved[k][...], preferred_element_type=F32)
            low, high = value[:, :HALF], value[:, HALF:]
            dsend[k][at, :] = jnp.where(c == 0, high, low).astype(BF16)
            send(dsend[k].at[at], drecv[k].at[at], give_d, base_d + i, sib)
            part[at, :] = jnp.where(c == 0, low, high)
        for i in range(PCH):
            finish(i)
        for h in range(1, parts):
            for q in range(chips):
                give_piece(q, h)
        between()
        sent.append((dsend[k], give_d, None))
        sent.append((arrived[k].at[:, 0:chips - 1], give_r, None))

        def total_of(h):
            at = pl.ds(pl.multiple_of(me * size + h * part_size, part_size), part_size)
            total = part[at, :] + drecv[k][at, :].astype(F32)
            wait_recv(arrived[k].at[h, 0:chips - 1], base_r + h)
            for i in range(1, chips):
                total = total + arrived[k][h, (me + i) % chips].astype(F32)
            return total

        return total_of

    def spread_level(k, total_of, between):
        chips = 2 * CHIPS[k]
        size = UR // CHIPS[k]
        u = ubuf[k]
        most = max(len(near) for near, _ in SPREAD[k])
        parts = PARTS[k]
        part_size = size // parts
        base_a, base_b = in_sem.take(most * parts), in_sem.take(3 * parts)
        base_f = in_sem.take()
        give, give_f = out_sem.take(), out_sem.take()

        def piece(mask, h):
            at = (flip(x, mask[0]) % 2) * 16 + flip(z, mask[1]) * 4 + flip(y, mask[2])
            at = at % chips * size + h * part_size
            return u.at[c, pl.ds(pl.multiple_of(at, part_size), part_size)]

        def across(ref):
            send(ref, ref, give_f, base_f, sib)

        for h in range(parts):
            own = piece((0, 0, 0), h)
            own[...] = total_of(h).astype(BF16)
            for core, (near, far) in enumerate(SPREAD[k]):
                @pl.when(c == core)
                def _():
                    for i, m in enumerate(near):
                        send(own, own, give, base_a + h * most + i, dev(m))
                    for j, m in enumerate(far):
                        send(own, own, give, base_b + h * 3 + j, dev(m))
                    across(own)

        for core, (near, far) in enumerate(SPREAD[k]):
            @pl.when(c == core)
            def _():
                for h in range(parts):
                    for i in reversed(range(len(near))):
                        ref = piece(near[i], h)
                        wait_recv(ref, base_a + h * most + i)
                        for j, m in enumerate(far):
                            send(ref, ref, give, base_b + h * 3 + j, dev(m))
                        across(ref)

        between()
        for core, (near, far) in enumerate(SPREAD[k]):
            @pl.when(c == core)
            def _():
                for h in range(parts):
                    for j in reversed(range(len(far))):
                        wait_recv(u.at[c, 0:(len(near) + 1) * part_size], base_b + h * 3 + j)
                        for m in ((0, 0, 0),) + near:
                            across(piece(xor(m, far[j]), h))

        sent.append((u.at[c, 0:(chips - 1) * size], give, None))
        sent.append((u.at[c], give_f, None))
        wait_recv(u.at[1 - c], base_f)
        rhs = jnp.concatenate([u[0], u[1]], axis=1)
        value = acc_l[k + 1][...] - jnp.dot(cols[k + 1][...], rhs, preferred_element_type=F32)
        solved[k + 1][...] = value.astype(BF16)
        out_copies.append(fetch(solved[k + 1], outs[k + 1]))

    def in_reduce(k):
        def run():
            if k == 0:
                for j in (2, 3):
                    pan_copy[j].wait()
                    pan[j][...] = pan_t[j][...].T
                l_step(2, 1, y == 3)
                l_step(3, 1, y == 3)
                l_collect(1, 1)
            if k == 1:
                l_step(3, 3)
            if k < 3:
                gather_columns(k + 1)
        return run

    def in_spread(k):
        def run():
            if k == 0:
                l_step(2, 2)
                l_step(3, 2)
            else:
                l_collect(k + 1, len(GATHER[k + 1][0]) - 1)
            l_finish(k + 1)
            l_product(k + 1)
        return run

    l_step(2, 1, y < 3)
    l_step(3, 1, y < 3)
    for k in range(4):
        total_of = update_level(k, in_reduce(k))
        if k < 3:
            spread_level(k, total_of, in_spread(k))

    fin_acc[...] = total_of(0)
    own_rows = fin_acc[pl.ds(pl.multiple_of(c * 24, 8), 24), :]
    fin_send[...] = fin_acc[pl.ds(pl.multiple_of((1 - c) * 24, 8), 24), :]
    si, ri = out_sem.take(), in_sem.take()
    send(fin_send, fin_recv, si, ri, sib)
    sent.append((fin_send, si, None))
    wait_recv(fin_recv, ri)
    other_rows = fin_recv[...]
    anc[:, :HALF] = jnp.where(c == 0, own_rows, other_rows)
    anc[:, HALF:] = jnp.where(c == 0, other_rows, own_rows)
    out_copies.append(fetch(anc, out_anc))
    for src, si, cond in sent:
        if cond is None:
            wait_send(src, si)
        else:
            pl.when(cond)(lambda src=src, si=si: wait_send(src, si))
    for copy in out_copies:
        copy.wait()
    assert (out_sem.used, in_sem.used, local.used) == (N_SEND, N_RECV, N_LOCAL)


def hand_over(*refs):
    given, taken, held, sem = refs[:5], refs[5:10], refs[10:15], refs[15]
    ins = [pltpu.make_async_copy(a, b, sem.at[i]) for i, (a, b) in enumerate(zip(given, held))]
    outs = [pltpu.make_async_copy(a, b, sem.at[5 + i]) for i, (a, b) in enumerate(zip(held, taken))]
    for copy in ins:
        copy.start()
    for first, second in zip(ins, outs):
        first.wait()
        second.start()
    for copy in outs:
        copy.wait()


def per_device(*args):
    vmem = pltpu.VMEM
    scratch = [vmem((ROWS[0], S), BF16)] + [vmem((SB, r, BLK), BF16) for r in ROWS[1:]]
    scratch += [vmem((UR, r), BF16) for r in ROWS]
    scratch += [vmem((4, 2, ROWS[0], N), BF16)]
    scratch += [vmem((NX[k], NZ[k], 4, 2, ROWS[k], N), BF16) for k in (1, 2, 3)]
    scratch += [vmem((2, 2 * UR, HALF), BF16) for _ in range(3)]
    scratch += [vmem((r, N), BF16) for r in ROWS]
    scratch += [vmem((ROWS[0], N), F32)]
    scratch += [vmem((ROWS[k], N), F32) for k in (1, 2, 3)]
    scratch += [vmem((ROWS[k], 2 * UR), BF16) for k in (1, 2, 3)]
    scratch += [vmem((UR, HALF), F32)]
    scratch += [vmem((UR, HALF), BF16)] * 12
    scratch += [vmem((p, n, UR // n // p, HALF), BF16) for n, p in zip(CHIPS, PARTS)]
    scratch += [vmem((ROWS[k], UR), BF16) for k in (2, 3)]
    scratch += [vmem((48, HALF), F32), vmem((24, HALF), F32), vmem((24, HALF), F32), vmem((24, N), F32)]
    scratch += [
        pltpu.SemaphoreType.DMA((N_SEND,)),
        pltpu.SemaphoreType.DMA((N_RECV,)),
        pltpu.SemaphoreType.DMA((N_LOCAL,)),
    ]
    anywhere = pl.BlockSpec(memory_space=pl.ANY)
    shapes = tuple(jax.ShapeDtypeStruct((r, N), BF16) for r in ROWS)
    shapes += (jax.ShapeDtypeStruct((24, N), F32),)
    args = args[:10] + (args[10].T, args[11].T) + args[12:]
    results = pl.pallas_call(
        kernel,
        out_shape=shapes,
        in_specs=[anywhere] * 12 + [pl.BlockSpec(memory_space=pltpu.SMEM)] * 3,
        out_specs=(anywhere,) * 5,
        scratch_shapes=scratch,
        compiler_params=pltpu.CompilerParams(
            collective_id=0, has_side_effects=True, vmem_limit_bytes=63 * 1024 * 1024
        ),
    )(*args)
    return pl.pallas_call(
        hand_over,
        out_shape=shapes,
        in_specs=[anywhere] * 5,
        out_specs=(anywhere,) * 5,
        scratch_shapes=[vmem(a.shape, a.dtype) for a in shapes] + [pltpu.SemaphoreType.DMA((10,))],
    )(*results)


def solution(mesh):
    split = P(("leaf", "rows"), None)
    in_specs = (split,) * 8 + (P(None, ("leaf", "rows")),) * 4 + (P(),) * 3
    return jax.shard_map(
        per_device, mesh=mesh, in_specs=in_specs, out_specs=(split,) * 5, check_vma=False
    )
```

```python
import jax
import jax.numpy as jnp
from jax import lax
from jax.experimental import pallas as pl
from jax.experimental.pallas import tpu as pltpu
from jax.sharding import PartitionSpec as P

S = 6144
N = 256
UR = 1536
BLK = 128
UB = 12
SB = S // BLK
HALF = 128
ROWS = (768, 384, 192, 96)
MESH = pl.DeviceIdType.MESH
F32 = jnp.float32
BF16 = jnp.bfloat16

STAGE = {
    "y": ((0, 0, 2), (0, 0, 1), (0, 0, 3)),
    "z1": ((0, 1, 0),),
    "z3": ((0, 3, 0),),
    "x1": ((1, 0, 0),),
}

CHIPS = (4, 8, 16, 32)

GATHER = {1: ("y", "z1"), 2: ("y", "z1", "z3"), 3: ("y", "z3", "z1", "x1")}
Y_MASKS = STAGE["y"]
Z_MASKS = ((0, 2, 0), (0, 1, 0), (0, 3, 0))
SPREAD = (
    ((((0, 1, 0),), Y_MASKS), (Y_MASKS, ((0, 1, 0),))),
    ((Z_MASKS, Y_MASKS), (Y_MASKS, Z_MASKS)),
    (
        (tuple((1,) + m[1:] for m in Z_MASKS) + Z_MASKS + ((1, 0, 0),), Y_MASKS),
        (tuple((1,) + m[1:] for m in Y_MASKS) + Y_MASKS + ((1, 0, 0),), Z_MASKS),
    ),
)
NX = {1: 1, 2: 1, 3: 2}
NZ = {1: 2, 2: 4, 3: 4}
NCH = 3
PCH = 4
PARTS = (4, 2, 2, 1)


def flip(value, mask):
    if mask == 0:
        return value
    if mask == 1:
        return value + 1 - 2 * (value % 2)
    if mask == 2:
        return (value + 2) % 4
    return 3 - value


def xor(a, b):
    return tuple(i ^ j for i, j in zip(a, b))


def held_before(order, step):
    held = [(0, 0, 0)]
    for name in order[:step]:
        held = held + [xor(h, m) for m in STAGE[name] for h in held]
    return held


def mask_id(mask):
    return mask[0] * 16 + mask[1] * 4 + mask[2]


class Counter:
    def __init__(self):
        self.used = 0

    def take(self, count=1):
        first = self.used
        self.used += count
        return first


N_SEND = 35
N_RECV = 110
N_LOCAL = 17


def kernel(*refs):
    loads = refs[0:4]
    inverse = refs[4:8]
    panel = refs[8:12]
    tables = (None,) + tuple(refs[12:15])
    outs = refs[15:19]
    out_anc = refs[19]
    scratch = list(refs[20:])

    def pop(count):
        taken = scratch[:count]
        del scratch[:count]
        return taken

    inv = pop(4)
    pan = pop(4)
    first = pop(1)[0]
    lbuf = [None] + pop(3)
    ubuf = pop(3)
    solved = pop(4)
    acc0 = pop(1)[0]
    acc_l = [None] + pop(3)
    cols = [None] + pop(3)
    part = pop(1)[0]
    dsend = pop(4)
    drecv = pop(4)
    stage = pop(4)
    arrived = pop(4)
    pan_t = [None, None] + pop(2)
    fin_acc, fin_send, fin_recv, anc = pop(4)
    ssem, rsem, lsem = pop(3)

    leaf = lax.axis_index("leaf")
    rows = lax.axis_index("rows")
    x, z, y, c = leaf // 4, leaf % 4, rows // 2, rows % 2
    out_sem = Counter()
    in_sem = Counter()
    local = Counter()
    sent = []

    def dev(mask, other_core=False):
        core = 1 - c if other_core else c
        return (flip(x, mask[0]) * 4 + flip(z, mask[1]), flip(y, mask[2]) * 2 + core)

    sib = dev((0, 0, 0), True)

    def send(src, dst, si, ri, device):
        pltpu.make_async_remote_copy(
            src_ref=src, dst_ref=dst, send_sem=ssem.at[si], recv_sem=rsem.at[ri],
            device_id=device, device_id_type=MESH,
        ).start()

    def wait_recv(dst, ri):
        pltpu.make_async_remote_copy(
            src_ref=dst, dst_ref=dst, send_sem=ssem.at[0], recv_sem=rsem.at[ri],
            device_id=sib, device_id_type=MESH,
        ).wait_recv()

    def wait_send(src, si):
        pltpu.make_async_remote_copy(
            src_ref=src, dst_ref=src, send_sem=ssem.at[si], recv_sem=rsem.at[0],
            device_id=sib, device_id_type=MESH,
        ).wait_send()

    def fetch(src, dst):
        copy = pltpu.make_async_copy(src, dst, lsem.at[local.take()])
        copy.start()
        return copy

    def fetch_blocks(k):
        sem = lsem.at[local.take()]
        for t in range(SB):
            pltpu.make_async_copy(
                inverse[k].at[:, t * BLK:(t + 1) * BLK], inv[k].at[t], sem
            ).start()
        return pltpu.make_async_copy(inv[k], inv[k], sem)

    barrier = pltpu.get_barrier_semaphore()
    hops = (0, 1, 2, 1)
    others = [(xm, zm, ym) for xm in range(2) for zm in range(4) for ym in range(4)][1:]
    others.sort(key=lambda m: -(m[0] + hops[m[1]] + hops[m[2]]))
    partners = [dev(m) for m in others] + [sib]
    for partner in partners:
        pl.semaphore_signal(barrier, inc=1, device_id=partner, device_id_type=MESH)
    own_first = fetch(loads[0], first.at[y, c])
    inv_copy = [fetch(inverse[0], inv[0])]
    pan_copy = [fetch(panel[0], pan[0])]
    for k in (1, 2, 3):
        inv_copy.append(fetch_blocks(k))
        pan_copy.append(fetch(panel[k], pan[k] if k == 1 else pan_t[k]))
    pl.semaphore_wait(barrier, len(partners))

    ch_rows = ROWS[0] // NCH
    g_recv = {m: in_sem.take(NCH) for m in (1, 2, 3)}
    g_fwd = {m: in_sem.take() for m in (0, 1, 2, 3)}
    g_send = {m: out_sem.take() for m in (1, 3)}
    g_relay = {m: out_sem.take() for m in (1, 3)}
    g_fsend = {m: out_sem.take() for m in (0, 1, 2, 3)}

    def first_at(mask, ch, core):
        return first.at[flip(y, mask), core, pl.ds(ch * ch_rows, ch_rows)]

    def below(mask):
        return flip(y, mask) < y

    def passes_on(core, block):
        return (c == core) & (block < flip(block, 2))

    l_recv = {k: in_sem.take(len(GATHER[k])) for k in (1, 2, 3)}
    l_fwd = {k: in_sem.take() for k in (1, 2, 3)}
    l_send = {k: out_sem.take(len(GATHER[k])) for k in (1, 2, 3)}
    l_fsend = {k: out_sem.take() for k in (1, 2, 3)}

    def l_bulk(k, step):
        ref = lbuf[k]
        count = len(STAGE[GATHER[k][step]]) * len(held_before(GATHER[k], step))
        if count == 3:
            return ref.at[0, 0, 0:3, 0]
        if count == 4:
            return ref.at[0, 0, :, 0]
        if count == 8:
            return ref.at[0, 0:2, :, 0]
        return ref.at[0, :, :, 0]

    def l_at(k, mask, core):
        xi = flip(x, mask[0]) % 2 if k == 3 else 0
        zi = flip(z, mask[1]) % NZ[k]
        return lbuf[k].at[xi, zi, flip(y, mask[2]), core]

    def l_source(k, mask):
        return loads[k] if mask == (0, 0, 0) else l_at(k, mask, c)

    def l_step(k, step, cond=None):
        def run():
            if step > 0:
                l_collect(k, step - 1)
            for mask in STAGE[GATHER[k][step]]:
                for held in held_before(GATHER[k], step):
                    send(l_source(k, held), l_at(k, held, c), l_send[k] + step, l_recv[k] + step,
                         dev(mask))

        if cond is None:
            run()
        else:
            pl.when(cond)(run)
        if (k, step) not in l_done:
            sent.append((l_bulk(k, step), l_send[k] + step, None))
        l_done.add((k, step))

    def l_collect(k, step):
        wait_recv(l_bulk(k, step), l_recv[k] + step)
        for mask in STAGE[GATHER[k][step]]:
            for held in held_before(GATHER[k], step):
                ref = l_at(k, xor(held, mask), c)
                send(ref, ref, l_fsend[k], l_fwd[k], sib)

    l_own = {}
    l_done = set()

    def l_begin(k):
        own = l_at(k, (0, 0, 0), c)
        send(loads[k], own, l_fsend[k], l_fwd[k], sib)
        l_own[k] = fetch(loads[k], own)
        sent.append((lbuf[k].at[:, :, :, 0], l_fsend[k], None))

    def l_finish(k):
        l_own[k].wait()
        wait_recv(lbuf[k].at[:, :, :, 1 - c], l_fwd[k])

    def l_product(k):
        whole = jnp.concatenate([inv[k][t] for t in range(SB)], axis=1)
        acc_l[k][...] = jnp.dot(
            whole, lbuf[k][...].reshape(S, N), preferred_element_type=F32
        )

    def gather_columns(k):
        inv_copy[k].wait()
        parent = leaf // (2 ** k)
        for j in range(2):
            for i in range(UB):
                t = tables[k][2 * parent + j, i]
                at = j * UR + i * BLK
                cols[k][:, at:at + BLK] = inv[k][t]

    l_step(1, 0)
    for m, core in ((1, 0), (3, 1)):
        wanted = (y < flip(y, m)) | passes_on(core, y)

        @pl.when(wanted)
        def _():
            for ch in range(NCH):
                src = loads[0].at[pl.ds(ch * ch_rows, ch_rows)]
                send(src, first_at(0, ch, c), g_send[m], g_recv[m] + ch, dev((0, 0, m)))

        sent.append((loads[0], g_send[m], wanted))

    @pl.when(c == 0)
    def _():
        send(loads[0], first.at[y, c], g_fsend[0], g_fwd[0], sib)

    sent.append((loads[0], g_fsend[0], c == 0))
    for k in (1, 2, 3):
        l_begin(k)

    def multiply(mask, same_core):
        yy = flip(y, mask)
        core = c if same_core else 1 - c
        col = pl.multiple_of((2 * yy + core) * ROWS[0], ROWS[0])
        acc0[...] += jnp.dot(
            inv[0][:, pl.ds(col, ROWS[0])], first[yy, core], preferred_element_type=F32
        )

    def g_take(mask, ch):
        needed = below(mask)
        block = flip(y, mask)
        core, onward = (0, 3) if mask == 1 else (1, 1)
        ref = first_at(mask, ch, c)
        relayed = passes_on(core, block) if mask != 2 else False

        @pl.when(needed | relayed)
        def _():
            wait_recv(ref, g_recv[mask] + ch)

        if mask != 2:
            @pl.when(relayed)
            def _():
                send(ref, ref, g_relay[mask], g_recv[2] + ch, dev((0, 0, onward)))

        @pl.when(needed)
        def _():
            send(ref, ref, g_fsend[mask], g_fwd[mask], sib)

        if ch == 0:
            if mask != 2:
                sent.append((loads[0], g_relay[mask], relayed))
            sent.append((loads[0], g_fsend[mask], needed))

    def g_multiply(mask):
        @pl.when(below(mask))
        def _():
            multiply(mask, True)
            wait_recv(first.at[flip(y, mask), 1 - c], g_fwd[mask])
            multiply(mask, False)

    acc0[...] = jnp.zeros_like(acc0)
    own_first.wait()
    inv_copy[0].wait()
    multiply(0, True)

    @pl.when(c == 1)
    def _():
        wait_recv(first.at[y, 1 - c], g_fwd[0])
        multiply(0, False)

    l_step(1, 1)
    for ch in range(NCH):
        g_take(1, ch)
        g_take(3, ch)
    l_step(2, 0)
    l_step(3, 0)
    g_multiply(1)
    g_multiply(3)
    for ch in range(NCH):
        g_take(2, ch)
    g_multiply(2)
    solved[0][...] = acc0[...].astype(BF16)
    out_copies = [fetch(solved[0], outs[0])]

    def place_of(k):
        return ((x % 2) * 16 + z * 4 + y) % CHIPS[k]

    def chip_of(k, place):
        whole = (x % 2) * 16 + z * 4 + y
        at = whole - whole % CHIPS[k] + place
        return ((x - x % 2 + at // 16) * 4 + (at // 4) % 4, (at % 4) * 2 + c)

    def update_level(k, between):
        chips, me = CHIPS[k], place_of(k)
        size = UR // chips
        if k < 2:
            pan_copy[k].wait()
        parts = PARTS[k]
        part_size = size // parts
        base_d, base_r = in_sem.take(PCH), in_sem.take(parts)
        give_d, give_r = out_sem.take(), out_sem.take()
        rows_of = UR // PCH

        def finish(i):
            at = pl.ds(i * rows_of, rows_of)
            wait_recv(drecv[k].at[at], base_d + i)
            stage[k][at, :] = (part[at, :] + drecv[k][at, :].astype(F32)).astype(BF16)
            for q in range(i * chips // PCH, (i + 1) * chips // PCH):
                give_piece(q, 0)

        def give_piece(q, h):
            @pl.when(q != me)
            def _():
                send(stage[k].at[pl.ds(q * size + h * part_size, part_size)],
                     arrived[k].at[h, me], give_r, base_r + h, chip_of(k, q))

        for i in range(PCH):
            at = pl.ds(i * rows_of, rows_of)
            value = jnp.dot(pan[k][at, :], solved[k][...], preferred_element_type=F32)
            low, high = value[:, :HALF], value[:, HALF:]
            dsend[k][at, :] = jnp.where(c == 0, high, low).astype(BF16)
            send(dsend[k].at[at], drecv[k].at[at], give_d, base_d + i, sib)
            part[at, :] = jnp.where(c == 0, low, high)
        for i in range(PCH):
            finish(i)
        for h in range(1, parts):
            for q in range(chips):
                give_piece(q, h)
        between()
        sent.append((dsend[k], give_d, None))
        sent.append((arrived[k].at[:, 0:chips - 1], give_r, None))

        def total_of(h):
            at = pl.ds(pl.multiple_of(me * size + h * part_size, part_size), part_size)
            total = part[at, :] + drecv[k][at, :].astype(F32)
            wait_recv(arrived[k].at[h, 0:chips - 1], base_r + h)
            for i in range(1, chips):
                total = total + arrived[k][h, (me + i) % chips].astype(F32)
            return total

        return total_of

    def spread_level(k, total_of, between):
        chips = 2 * CHIPS[k]
        size = UR // CHIPS[k]
        u = ubuf[k]
        most = max(len(near) for near, _ in SPREAD[k])
        parts = PARTS[k]
        part_size = size // parts
        base_a, base_b = in_sem.take(most * parts), in_sem.take(3 * parts)
        base_f = in_sem.take()
        give, give_f = out_sem.take(), out_sem.take()

        def piece(mask, h):
            at = (flip(x, mask[0]) % 2) * 16 + flip(z, mask[1]) * 4 + flip(y, mask[2])
            at = at % chips * size + h * part_size
            return u.at[c, pl.ds(pl.multiple_of(at, part_size), part_size)]

        def across(ref):
            send(ref, ref, give_f, base_f, sib)

        for h in range(parts):
            own = piece((0, 0, 0), h)
            own[...] = total_of(h).astype(BF16)
            for core, (near, far) in enumerate(SPREAD[k]):
                @pl.when(c == core)
                def _():
                    for i, m in enumerate(near):
                        send(own, own, give, base_a + h * most + i, dev(m))
                    for j, m in enumerate(far):
                        send(own, own, give, base_b + h * 3 + j, dev(m))
                    across(own)

        for core, (near, far) in enumerate(SPREAD[k]):
            @pl.when(c == core)
            def _():
                for h in range(parts):
                    for i in reversed(range(len(near))):
                        ref = piece(near[i], h)
                        wait_recv(ref, base_a + h * most + i)
                        for j, m in enumerate(far):
                            send(ref, ref, give, base_b + h * 3 + j, dev(m))
                        across(ref)

        between()
        for core, (near, far) in enumerate(SPREAD[k]):
            @pl.when(c == core)
            def _():
                for h in range(parts):
                    for j in reversed(range(len(far))):
                        wait_recv(u.at[c, 0:(len(near) + 1) * part_size], base_b + h * 3 + j)
                        for m in ((0, 0, 0),) + near:
                            across(piece(xor(m, far[j]), h))

        sent.append((u.at[c, 0:(chips - 1) * size], give, None))
        sent.append((u.at[c], give_f, None))
        wait_recv(u.at[1 - c], base_f)
        rhs = jnp.concatenate([u[0], u[1]], axis=1)
        value = acc_l[k + 1][...] - jnp.dot(cols[k + 1][...], rhs, preferred_element_type=F32)
        solved[k + 1][...] = value.astype(BF16)
        out_copies.append(fetch(solved[k + 1], outs[k + 1]))

    def in_reduce(k):
        def run():
            if k == 0:
                for j in (2, 3):
                    pan_copy[j].wait()
                    pan[j][...] = pan_t[j][...].T
                l_step(2, 1, y == 3)
                l_step(3, 1, y == 3)
                l_collect(1, 1)
            if k == 1:
                l_step(3, 3)
            if k < 3:
                gather_columns(k + 1)
        return run

    def in_spread(k):
        def run():
            if k == 0:
                l_step(2, 2)
                l_step(3, 2)
            else:
                l_collect(k + 1, len(GATHER[k + 1]) - 1)
            l_finish(k + 1)
            l_product(k + 1)
        return run

    l_step(2, 1, y < 3)
    l_step(3, 1, y < 3)
    for k in range(4):
        total_of = update_level(k, in_reduce(k))
        if k < 3:
            spread_level(k, total_of, in_spread(k))

    fin_acc[...] = total_of(0)
    own_rows = fin_acc[pl.ds(pl.multiple_of(c * 24, 8), 24), :]
    fin_send[...] = fin_acc[pl.ds(pl.multiple_of((1 - c) * 24, 8), 24), :]
    si, ri = out_sem.take(), in_sem.take()
    send(fin_send, fin_recv, si, ri, sib)
    sent.append((fin_send, si, None))
    wait_recv(fin_recv, ri)
    other_rows = fin_recv[...]
    anc[:, :HALF] = jnp.where(c == 0, own_rows, other_rows)
    anc[:, HALF:] = jnp.where(c == 0, other_rows, own_rows)
    out_copies.append(fetch(anc, out_anc))
    for src, si, cond in sent:
        if cond is None:
            wait_send(src, si)
        else:
            pl.when(cond)(lambda src=src, si=si: wait_send(src, si))
    for copy in out_copies:
        copy.wait()
    assert (out_sem.used, in_sem.used, local.used) == (N_SEND, N_RECV, N_LOCAL)


def hand_over(*refs):
    given, taken, held, sem = refs[:5], refs[5:10], refs[10:15], refs[15]
    ins = [pltpu.make_async_copy(a, b, sem.at[i]) for i, (a, b) in enumerate(zip(given, held))]
    outs = [pltpu.make_async_copy(a, b, sem.at[5 + i]) for i, (a, b) in enumerate(zip(held, taken))]
    for copy in ins:
        copy.start()
    for first, second in zip(ins, outs):
        first.wait()
        second.start()
    for copy in outs:
        copy.wait()


def per_device(*args):
    vmem = pltpu.VMEM
    scratch = [vmem((ROWS[0], S), BF16)] + [vmem((SB, r, BLK), BF16) for r in ROWS[1:]]
    scratch += [vmem((UR, r), BF16) for r in ROWS]
    scratch += [vmem((4, 2, ROWS[0], N), BF16)]
    scratch += [vmem((NX[k], NZ[k], 4, 2, ROWS[k], N), BF16) for k in (1, 2, 3)]
    scratch += [vmem((2, 2 * UR, HALF), BF16) for _ in range(3)]
    scratch += [vmem((r, N), BF16) for r in ROWS]
    scratch += [vmem((ROWS[0], N), F32)]
    scratch += [vmem((ROWS[k], N), F32) for k in (1, 2, 3)]
    scratch += [vmem((ROWS[k], 2 * UR), BF16) for k in (1, 2, 3)]
    scratch += [vmem((UR, HALF), F32)]
    scratch += [vmem((UR, HALF), BF16)] * 12
    scratch += [vmem((p, n, UR // n // p, HALF), BF16) for n, p in zip(CHIPS, PARTS)]
    scratch += [vmem((ROWS[k], UR), BF16) for k in (2, 3)]
    scratch += [vmem((48, HALF), F32), vmem((24, HALF), F32), vmem((24, HALF), F32), vmem((24, N), F32)]
    scratch += [
        pltpu.SemaphoreType.DMA((N_SEND,)),
        pltpu.SemaphoreType.DMA((N_RECV,)),
        pltpu.SemaphoreType.DMA((N_LOCAL,)),
    ]
    anywhere = pl.BlockSpec(memory_space=pl.ANY)
    shapes = tuple(jax.ShapeDtypeStruct((r, N), BF16) for r in ROWS)
    shapes += (jax.ShapeDtypeStruct((24, N), F32),)
    args = args[:10] + (args[10].T, args[11].T) + args[12:]
    results = pl.pallas_call(
        kernel,
        out_shape=shapes,
        in_specs=[anywhere] * 12 + [pl.BlockSpec(memory_space=pltpu.SMEM)] * 3,
        out_specs=(anywhere,) * 5,
        scratch_shapes=scratch,
        compiler_params=pltpu.CompilerParams(
            collective_id=0, has_side_effects=True, vmem_limit_bytes=63 * 1024 * 1024
        ),
    )(*args)
    return pl.pallas_call(
        hand_over,
        out_shape=shapes,
        in_specs=[anywhere] * 5,
        out_specs=(anywhere,) * 5,
        scratch_shapes=[vmem(a.shape, a.dtype) for a in shapes] + [pltpu.SemaphoreType.DMA((10,))],
    )(*results)


def solution(mesh):
    split = P(("leaf", "rows"), None)
    in_specs = (split,) * 8 + (P(None, ("leaf", "rows")),) * 4 + (P(),) * 3
    return jax.shard_map(
        per_device, mesh=mesh, in_specs=in_specs, out_specs=(split,) * 5, check_vma=False
    )
```
